32 devices in a mesh: mp: 8 (over z, x), dp: 4 (over y, core).
Axes of the slice: x: 2, y: 2, z: 4, core: 2. Of those that a mesh axis runs over, the one named last changes fastest.
Arguments:
- tables: bfloat16 [20, 16384, 128], P(None, 'mp'), may hold values from -3 to 3
- block_rows: int32 [2048, 128], P(('mp', 'dp')), may hold values from 0 to 2047
- block_slots: int32 [2048, 128], P(('mp', 'dp')), may hold values from 0 to 127
- block_table: int32 [2048], P(('mp', 'dp')), may hold values from 0 to 19
- block_peer: int32 [2048, 1], P(('mp', 'dp')), may hold values from 0 to 7; in each aligned block of 64 rows (0 to 63, 64 to 127, ...) at most 16 rows name the same one
- block_len: int32 [2048], P(('mp', 'dp')), may hold values from 1 to 128
- block_count: int32 [32], P(('mp', 'dp')), may hold values from 1 to 64, as said below
- cross_in: bfloat16 [4, 2560, 256], P(None, 'dp'), may hold values from -0.23632812 to 0.23632812
- cross_mix: bfloat16 [4, 256, 256], replicated, may hold values from -0.5625 to 0.5625
- cross_out: bfloat16 [4, 256, 2560], P(None, None, 'dp'), may hold values from -0.375 to 0.375
- cross_bias: float32 [4, 2560], replicated, may hold values from -3 to 3
- gate_weight: bfloat16 [4, 2560], replicated, may hold values from -0.47265625 to 0.47265625
Outputs:
- crossed: bfloat16 [4096, 2560], P(('mp', 'dp'))
The draws below stay inside these ranges and needn't reach their ends.
Inputs may be any that keep to these rules, and one draw needn't show every extreme that they name: `block_peer`: in the 64 blocks of one device no destination is named by more than 16 blocks, a bound that the blocks of some device reach. The live blocks of a device are its first block_count blocks; some device has exactly 64. Entries of a block at positions below its block_len are live. `block_rows`: A row index within the device's own shard of the table. `block_slots`: A sample of the destination device.
All inputs are finite; a program needn't handle non-finite values.
Results may differ from the reference program's by a relative error of at most 0.0059.
Values may be sent and summed in bfloat16 or wider, within the bound.
A program may use at most 128 MiB of HBM per device.

```python
import math
import jax
import jax.numpy as jnp
import numpy as np
from jax import lax

WIDTH = 128
TABLES = 20
ROWS_DEV = 2048
BLOCK = 128
NBLK = 64
B_DEV = 128
RANK = 256
EXPERTS = 4
D = 2560
CAP = 16
N_MP = 8
N_DP = 4


def draw_block_count(key, part):
    devices = N_MP * N_DP
    heavy = jax.random.randint(jax.random.fold_in(key, 11), (devices,), 0, 8) == 0
    high = jax.random.randint(jax.random.fold_in(key, 12), (devices,), NBLK // 2, NBLK + 1)
    low = jax.random.randint(jax.random.fold_in(key, 13), (devices,), max(1, NBLK // 8), NBLK // 2 + 1)
    counts = jnp.where(heavy, high, low)
    chosen = jax.random.randint(jax.random.fold_in(key, 14), (), 0, devices)
    return counts.at[chosen].set(NBLK).astype(jnp.int32)


def touch_ends(values, own_key, least, largest):
    extent = values.shape
    place = [jax.random.randint(jax.random.fold_in(own_key, axis), (), 0, extent[axis]) for axis in range(len(extent))]
    values = values.at[tuple(place)].set(least)
    longest = extent.index(max(extent))
    place[longest] = (place[longest] + 1) % extent[longest]
    return values.at[tuple(place)].set(largest)


def block_levels(key, extent, cuts, smallest, top_value):
    loudness = 1.0
    for dim, blocks in cuts:
        draws = jax.random.uniform(jax.random.fold_in(jax.random.fold_in(key, 6), dim), (blocks,), jnp.float32, smallest / len(cuts), top_value / len(cuts))
        loudness = loudness * jnp.repeat(jnp.exp(draws), extent[dim] // blocks).reshape((-1,) + (1,) * (len(extent) - 1 - dim))
    return loudness


def routed_block(key, own, number, rows, amount, top, bound, slope):
    order = jax.random.permutation(key, amount)
    packed, common = load_shares(amount, rows * top, bound, slope, True), load_shares(amount, rows * top, bound, slope, False)
    places = jnp.arange(amount)

    def named(tallies, rotation):
        used = int((tallies > 0).sum())
        fixed = max(1, used // 4)
        passed = fixed + (places - fixed + rotation * (used - fixed)) % max(1, amount - fixed)
        return jnp.zeros((amount,), jnp.int32).at[order[jnp.where(places < fixed, places, passed)]].set(jnp.asarray(tallies, jnp.int32))

    tallies = jnp.where(number % 4 == 0, named(packed, number // 4), named(common, number - number // 4 - 1))
    mixed = jax.random.permutation(jax.random.fold_in(own, 3), amount)
    donor, receiver = mixed[0:amount // 2 * 2:2], mixed[1:amount // 2 * 2:2]
    margin = jnp.minimum(tallies[donor] - 1, bound - tallies[receiver]) // 2
    margin = jnp.where((donor == order[0]) | (receiver == order[0]) | (tallies[receiver] == 0), 0, jnp.maximum(margin, 0))
    passed = jax.random.randint(jax.random.fold_in(own, 4), (amount // 2,), 0, 1 << 20) % (margin + 1)
    tallies = tallies.at[donor].add(-passed).at[receiver].add(passed)
    labels = jnp.searchsorted(jnp.cumsum(tallies), jnp.arange(rows * top), side="right").astype(jnp.int32)
    grid = labels.reshape(top, rows).T
    grid = grid[jax.random.permutation(jax.random.fold_in(own, 1), rows)]
    rotation = jax.random.randint(jax.random.fold_in(own, 2), (rows, 1), 0, top)
    return jnp.take_along_axis(grid, (jnp.arange(top)[None, :] + rotation) % top, axis=1)


def load_shares(count, total, reach, skew, full):
    weights = [(1 << 20) // math.isqrt(standing ** skew) + 1 for standing in range(1, count + 1)]
    largest = reach if full else min(reach, max(-(-total // count), total * weights[0] // sum(weights)))
    least = 1 if total - largest >= count - 1 else 0
    given, surplus = [largest] + [least] * (count - 1), total - largest - least * (count - 1)
    while surplus > 0:
        free = [i for i in range(1, count) if given[i] < largest] or [i for i in range(1, count) if given[i] < reach]
        whole, budget = sum([weights[i] for i in free]), surplus
        for i in free:
            extra = min(reach - given[i], max(1, budget * weights[i] // whole), surplus)
            given[i] = given[i] + extra
            surplus = surplus - extra
    return np.array(given)


def normal_values(stream_key, dims, deviation, limit, shards=(), kind=jnp.bfloat16):
    level = block_levels(stream_key, dims, shards, -0.22, 0.18) if shards else 1.0
    values = jax.random.normal(stream_key, dims, jnp.float32) * deviation * level
    return jnp.minimum(jnp.maximum(values, -limit), limit).astype(kind)


def setup_inputs(seed: int = 0) -> dict:
    key_list = jax.random.split(jax.random.key(seed), 13)
    tables = normal_values(key_list[0], (TABLES, ROWS_DEV * N_MP, WIDTH), 0.5, 3.0, ((1, 8),))
    block_rows = touch_ends(jax.random.randint(key_list[1], (N_MP * N_DP * NBLK, BLOCK), 0, ROWS_DEV), jax.random.fold_in(key_list[1], 1), 0, ROWS_DEV - 1).astype(jnp.int32)
    block_slots = touch_ends(jax.random.randint(key_list[2], (N_MP * N_DP * NBLK, BLOCK), 0, B_DEV), jax.random.fold_in(key_list[2], 1), 0, B_DEV - 1).astype(jnp.int32)
    block_table = touch_ends(jax.random.randint(key_list[3], (N_MP * N_DP * NBLK,), 0, TABLES), jax.random.fold_in(key_list[3], 1), 0, TABLES - 1).astype(jnp.int32)
    block_peer_keys = jax.random.split(jax.random.fold_in(key_list[4], 1), (N_MP * N_DP * NBLK) // NBLK)
    block_peer_turns = jax.random.permutation(jax.random.fold_in(key_list[4], 3), (N_MP * N_DP * NBLK) // NBLK)
    block_peer = jax.vmap(lambda own, number: routed_block(jax.random.fold_in(key_list[4], 2), own, number, NBLK, N_MP, 1, CAP, 2))(block_peer_keys, block_peer_turns).reshape((N_MP * N_DP * NBLK, 1))
    block_len = touch_ends(jax.random.randint(key_list[5], (N_MP * N_DP * NBLK,), 1, BLOCK + 1), jax.random.fold_in(key_list[5], 1), 1, BLOCK).astype(jnp.int32)
    block_count = draw_block_count(jax.random.fold_in(key_list[12], 71), 0)
    cross_in = normal_values(key_list[7], (EXPERTS, D, RANK), (2.0 / D ** 0.5), 0.23632812, ((1, 4),))
    cross_mix = normal_values(key_list[8], (EXPERTS, RANK, RANK), (1.5 / RANK ** 0.5), 0.5625)
    cross_out = normal_values(key_list[9], (EXPERTS, RANK, D), RANK ** -0.5, 0.375, ((2, 4),))
    cross_bias = normal_values(key_list[10], (EXPERTS, D), 0.5, 3.0, (), jnp.float32)
    gate_weight = normal_values(key_list[11], (EXPERTS, D), (4.0 / D ** 0.5), 0.47265625)
    return {"tables": tables, "block_rows": block_rows, "block_slots": block_slots, "block_table": block_table, "block_peer": block_peer, "block_len": block_len, "block_count": block_count, "cross_in": cross_in, "cross_mix": cross_mix, "cross_out": cross_out, "cross_bias": cross_bias, "gate_weight": gate_weight}


def reference(tables, block_rows, block_slots, block_table, block_peer, block_len, block_count, cross_in, cross_mix, cross_out, cross_bias, gate_weight):
    devices = N_MP * N_DP
    rows_all = block_rows.reshape(devices, NBLK, BLOCK)
    slots_all = block_slots.reshape(devices, NBLK, BLOCK)
    table_all = block_table.reshape(devices, NBLK)
    peer_all = block_peer.reshape(devices, NBLK)
    length_all = block_len.reshape(devices, NBLK)
    entries = jnp.arange(BLOCK, dtype=jnp.int32)
    blocks = jnp.arange(NBLK, dtype=jnp.int32)

    def one_device(index, total):
        shard = index // N_DP
        group = index % N_DP
        live = (blocks[:, None] < block_count[index]) & (entries[None, :] < length_all[index][:, None])
        table_ids = jnp.broadcast_to(table_all[index][:, None], (NBLK, BLOCK)).astype(jnp.int32)
        peer_ids = jnp.broadcast_to(peer_all[index][:, None], (NBLK, BLOCK)).astype(jnp.int32)
        row_ids = (rows_all[index] + shard * ROWS_DEV).astype(jnp.int32)
        values = tables[table_ids, row_ids].astype(jnp.float32) * live[:, :, None].astype(jnp.float32)
        partial_value = jnp.zeros((N_MP, TABLES, B_DEV, WIDTH), jnp.float32)
        partial_value = partial_value.at[peer_ids, table_ids, slots_all[index]].add(values)
        rounded = lax.optimization_barrier(partial_value.astype(jnp.bfloat16)).astype(jnp.float32)
        return total.at[:, group].add(rounded)

    total = lax.fori_loop(0, devices, one_device, jnp.zeros((N_MP, N_DP, TABLES, B_DEV, WIDTH), jnp.float32))
    embedded = total.transpose(0, 1, 3, 2, 4).reshape(devices * B_DEV, TABLES * WIDTH).astype(jnp.bfloat16)
    gate = jax.nn.sigmoid(jnp.dot(embedded, gate_weight.T, preferred_element_type=jnp.float32))
    weighted = jnp.zeros(embedded.shape, jnp.float32)
    for expert in range(EXPERTS):
        hidden = jnp.tanh(jnp.dot(embedded, cross_in[expert], preferred_element_type=jnp.float32)).astype(jnp.bfloat16)
        mixed = jnp.tanh(jnp.dot(hidden, cross_mix[expert], preferred_element_type=jnp.float32)).astype(jnp.bfloat16)
        expand = jnp.dot(mixed, cross_out[expert], preferred_element_type=jnp.float32) + cross_bias[expert][None, :]
        weighted = weighted + gate[:, expert][:, None] * expand
    base = embedded.astype(jnp.float32)
    return (base + base * weighted).astype(jnp.bfloat16)
```

```python
import functools

import jax
import jax.numpy as jnp
from jax import lax
from jax.experimental import pallas as pl
from jax.experimental.pallas import tpu as pltpu
from jax.sharding import PartitionSpec as P

B_DEV = 128
UNROLL = 8
STREAMS = 4
MESH = pl.DeviceIdType.MESH
POOL_LIMIT = 30 << 20
FUSED_LIMIT = 48 << 20
FOLD = 4
VMEM_LIMIT = 67043328


def pool_kernel(
    unroll,
    count_ref,
    table_hbm,
    peer_hbm,
    len_hbm,
    rows_hbm,
    slots_hbm,
    tables_hbm,
    out_ref,
    table_ref,
    peer_ref,
    len_ref,
    rows_ref,
    slots_ref,
    tables_ref,
    acc,
    slot_of,
    key_of,
    ready,
    small_sem,
    table_sem,
):
    table_count, rows_dev, width = tables_ref.shape
    total_blocks, block = rows_ref.shape
    tiles, samples, _ = out_ref.shape
    pairs = (
        (table_hbm, table_ref),
        (peer_hbm, peer_ref),
        (len_hbm, len_ref),
        (rows_hbm, rows_ref),
        (slots_hbm, slots_ref),
    )
    small = [pltpu.make_async_copy(a, b, small_sem.at[i]) for i, (a, b) in enumerate(pairs)]
    for copy in small:
        copy.start()

    def table_copy(t):
        return pltpu.make_async_copy(tables_hbm.at[t], tables_ref.at[t], table_sem.at[t])

    for t in range(table_count):
        table_copy(t).start()
        ready[t] = 0

    def need(t):
        @pl.when(ready[t] == 0)
        def _():
            table_copy(t).wait()
            ready[t] = 1

    def clear(i, carry):
        out_ref[i] = jnp.zeros((samples, width), jnp.bfloat16)
        slot_of[i] = -1
        return carry

    lax.fori_loop(0, tiles, clear, 0)
    for copy in small:
        copy.wait()
    count = count_ref[0]

    lane = lax.broadcasted_iota(jnp.int32, (block, 128), 1)
    sample = lax.broadcasted_iota(jnp.int32, (samples, block), 0)
    entry = lax.broadcasted_iota(jnp.int32, (samples, block), 1)

    def group(g, used):
        made = []
        for u in range(unroll):
            need(table_ref[g * unroll + u])
        for u in range(unroll):
            b = g * unroll + u
            row = rows_ref[pl.ds(b, 1), :]
            slot = slots_ref[pl.ds(b, 1), :]
            table = table_ref[b]
            column = jnp.broadcast_to(row, (128, block)).T
            pick = jnp.concatenate(
                [
                    jnp.where(column == lane + c * 128, 1.0, 0.0).astype(jnp.bfloat16)
                    for c in range(rows_dev // 128)
                ],
                axis=1,
            )
            picked = jnp.dot(pick, tables_ref[table], preferred_element_type=jnp.float32)
            place = jnp.where((sample == slot) & (entry < len_ref[b]), 1.0, 0.0)
            made.append(
                jnp.dot(
                    place.astype(jnp.bfloat16),
                    picked.astype(jnp.bfloat16),
                    preferred_element_type=jnp.float32,
                )
            )
        for u in range(unroll):
            b = g * unroll + u
            key = peer_ref[b] * table_count + table_ref[b]
            live = b < count
            known = slot_of[key]
            first = known < 0
            at = jnp.where(live, jnp.where(first, used, known), total_blocks)
            acc[at] = jnp.where(first, made[u], acc[at] + made[u])
            slot_of[key] = jnp.where(live, at, known)
            key_of[at] = key
            used = used + jnp.where(live & first, 1, 0)
        return used

    used = lax.fori_loop(0, (count + unroll - 1) // unroll, group, 0)

    def flush(i, carry):
        out_ref[key_of[i]] = acc[i].astype(jnp.bfloat16)
        return carry

    lax.fori_loop(0, used, flush, 0)
    for t in range(table_count):
        need(t)


def pool(peers, tables, block_rows, block_slots, block_table, block_peer, block_len, block_count):
    table_count, _, width = tables.shape
    total_blocks = block_rows.shape[0]
    tiles = peers * table_count
    unroll = UNROLL if total_blocks % UNROLL == 0 else 1
    hbm = pl.BlockSpec(memory_space=pltpu.HBM)
    vmem = pl.BlockSpec(memory_space=pltpu.VMEM)
    return pl.pallas_call(
        functools.partial(pool_kernel, unroll),
        out_shape=jax.ShapeDtypeStruct((tiles, B_DEV, width), jnp.bfloat16),
        in_specs=[pl.BlockSpec(memory_space=pltpu.SMEM)] + [hbm] * 6,
        out_specs=vmem,
        scratch_shapes=[
            pltpu.SMEM((total_blocks,), jnp.int32),
            pltpu.SMEM((total_blocks,), jnp.int32),
            pltpu.SMEM((total_blocks,), jnp.int32),
            pltpu.VMEM(block_rows.shape, jnp.int32),
            pltpu.VMEM(block_slots.shape, jnp.int32),
            pltpu.VMEM(tables.shape, jnp.bfloat16),
            pltpu.VMEM((total_blocks + 1, B_DEV, width), jnp.float32),
            pltpu.SMEM((tiles,), jnp.int32),
            pltpu.SMEM((total_blocks + 1,), jnp.int32),
            pltpu.SMEM((table_count,), jnp.int32),
            pltpu.SemaphoreType.DMA((5,)),
            pltpu.SemaphoreType.DMA((table_count,)),
        ],
        compiler_params=pltpu.CompilerParams(
            vmem_limit_bytes=POOL_LIMIT if peers <= 8 else VMEM_LIMIT
        ),
        cost_estimate=pl.CostEstimate(
            flops=2 * total_blocks * B_DEV * tables.shape[1] * width,
            bytes_accessed=2 * tables.size + 2 * tiles * B_DEV * width,
            transcendentals=0,
        ),
        name="pool",
    )(
        block_count,
        *(
            pltpu.with_memory_space_constraint(x, pltpu.HBM)
            for x in (
                block_table,
                block_peer[:, 0],
                block_len,
                block_rows,
                block_slots,
                tables,
            )
        )
    )


def cross_kernel(
    peers,
    partial_ref,
    in_ref,
    mix_ref,
    out_w_ref,
    bias_ref,
    gate_ref,
    result_ref,
    held,
    emb,
    ring_send,
    ring_recv,
):
    tiles, samples, width = partial_ref.shape
    table_count = tiles // peers
    part = table_count // STREAMS
    experts = mix_ref.shape[0]
    me = lax.axis_index("mp")
    half = peers // 2
    at = jnp.where(lax.rem(me, 2) == 0, lax.div(me, 2), peers - 1 - lax.div(me, 2))

    def member(position):
        position = lax.rem(position + 2 * peers, peers)
        return jnp.where(position < half, 2 * position, 2 * (peers - 1 - position) + 1)

    ahead, behind = member(at + 1), member(at - 1)

    barrier = pltpu.get_barrier_semaphore()
    greet = [{"mp": ahead}, {"mp": behind}]
    for target in greet:
        pl.semaphore_signal(barrier, inc=1, device_id=target, device_id_type=MESH)
    pl.semaphore_wait(barrier, len(greet))

    def ring_copy(stream, source, step):
        target = ahead if stream % 2 == 0 else behind
        return pltpu.make_async_remote_copy(
            src_ref=source,
            dst_ref=held.at[step, stream],
            send_sem=ring_send.at[stream, step],
            recv_sem=ring_recv.at[stream, step],
            device_id={"mp": target},
            device_id_type=MESH,
        )

    def own_tiles(stream, distance):
        dest = member(at - distance if stream % 2 == 0 else at + distance)
        return pl.ds(dest * table_count + stream * part, part)

    for stream in range(STREAMS):
        ring_copy(stream, partial_ref.at[own_tiles(stream, 1)], 0).start()

    def hop(step, last):
        for stream in range(STREAMS):
            ring_copy(stream, held.at[step, stream], step).wait_recv()
            mine = partial_ref[own_tiles(stream, step + 2)]
            total = held[step, stream].astype(jnp.float32) + mine.astype(jnp.float32)
            total = total.astype(jnp.bfloat16)
            if last:
                for i in range(part):
                    column = (stream * part + i) * width
                    emb[:, column : column + width] = total[i]
            else:
                held[step, stream] = total
                ring_copy(stream, held.at[step, stream], step + 1).start()

    def turn(step, carry):
        hop(step, False)
        return carry

    lax.fori_loop(0, peers - 2, turn, 0)
    hop(peers - 2, True)

    gate = jax.nn.sigmoid(
        lax.dot_general(
            emb[...], gate_ref[...], (((1,), (1,)), ((), ())), preferred_element_type=jnp.float32
        )
    )
    mixed = []
    for e in range(experts):
        projected = jnp.dot(emb[...], in_ref[e], preferred_element_type=jnp.float32)
        hidden = jnp.tanh(projected).astype(jnp.bfloat16)
        mixed.append(
            jnp.tanh(
                jnp.dot(hidden, mix_ref[e], preferred_element_type=jnp.float32)
            ).astype(jnp.bfloat16)
        )
    weighted = jnp.zeros(emb.shape, jnp.float32)
    for e in range(experts):
        grown = jnp.dot(mixed[e], out_w_ref[e], preferred_element_type=jnp.float32)
        weighted += gate[:, e : e + 1] * (grown + bias_ref[e : e + 1, :])
    base = emb[...].astype(jnp.float32)
    result_ref[...] = (base + base * weighted).astype(jnp.bfloat16)

    for stream in range(STREAMS):
        ring_copy(stream, partial_ref.at[own_tiles(stream, 1)], 0).wait_send()

    def sent(step, carry):
        for stream in range(STREAMS):
            ring_copy(stream, held.at[step - 1, stream], step).wait_send()
        return carry

    lax.fori_loop(1, peers - 1, sent, 0)


def plan_kernel(
    peers,
    count_ref,
    table_hbm,
    peer_hbm,
    len_hbm,
    rows_hbm,
    slots_hbm,
    rows_out,
    slots_out,
    index_ref,
    table_ref,
    peer_ref,
    len_ref,
    rows_ref,
    slots_ref,
    near_ref,
    small_sem,
):
    blocks, block = rows_out.shape
    tiles = index_ref.shape[0] - 2 * blocks
    table_count = tiles // peers
    part = table_count // STREAMS
    pairs = (
        (table_hbm, table_ref),
        (peer_hbm, peer_ref),
        (len_hbm, len_ref),
        (rows_hbm, rows_ref),
        (slots_hbm, slots_ref),
    )
    small = [pltpu.make_async_copy(a, b, small_sem.at[i]) for i, (a, b) in enumerate(pairs)]
    for copy in small:
        copy.start()
    me = lax.axis_index("mp")
    at = jnp.where(lax.rem(me, 2) == 0, lax.div(me, 2), peers - 1 - lax.div(me, 2))

    def clear(i, carry):
        index_ref[2 * blocks + i] = blocks
        return carry

    lax.fori_loop(0, tiles, clear, 0, unroll=8)
    for copy in small:
        copy.wait()
    count = count_ref[0]

    def look(b, found):
        peer = peer_ref[b]
        place = jnp.where(lax.rem(peer, 2) == 0, lax.div(peer, 2), peers - 1 - lax.div(peer, 2))
        forward = lax.rem(lax.div(table_ref[b], part), 2) == 0
        away = jnp.where(forward, at - place, place - at)
        near = (b < count) & ((away == 1) | (away == 1 - peers))
        near = jnp.where(near, 1, 0)
        near_ref[b] = near
        return found + near

    found = lax.fori_loop(0, blocks, look, 0, unroll=8)
    lane = lax.broadcasted_iota(jnp.int32, (1, block), 1)

    def settle(b, carry):
        low, high = carry
        near = near_ref[b]
        table = table_ref[b]
        live = b < count
        spot = jnp.where(near == 1, low, high)
        rows_out[pl.ds(spot, 1), :] = rows_ref[pl.ds(b, 1), :]
        length = jnp.where(live, len_ref[b], 0)
        slots_out[pl.ds(spot, 1), :] = jnp.where(lane < length, slots_ref[pl.ds(b, 1), :], -1)
        index_ref[spot] = table
        key = 2 * blocks + peer_ref[b] * table_count + table
        known = index_ref[key]
        index_ref[blocks + spot] = jnp.where(live, known, blocks)
        index_ref[key] = jnp.where(live, spot, known)
        return low + near, high + 1 - near

    lax.fori_loop(0, blocks, settle, (0, found), unroll=4)


def plan(peers, table_count, block_rows, block_slots, block_table, block_peer, block_len, block_count):
    blocks = block_rows.shape[0]
    hbm = pl.BlockSpec(memory_space=pltpu.HBM)
    vmem = pl.BlockSpec(memory_space=pltpu.VMEM)
    smem = pl.BlockSpec(memory_space=pltpu.SMEM)
    return pl.pallas_call(
        functools.partial(plan_kernel, peers),
        out_shape=(
            jax.ShapeDtypeStruct(block_rows.shape, jnp.int32),
            jax.ShapeDtypeStruct(block_slots.shape, jnp.int32),
            jax.ShapeDtypeStruct((2 * blocks + peers * table_count,), jnp.int32),
        ),
        in_specs=[smem] + [hbm] * 5,
        out_specs=(vmem, vmem, smem),
        scratch_shapes=[
            pltpu.SMEM((blocks,), jnp.int32),
            pltpu.SMEM((blocks,), jnp.int32),
            pltpu.SMEM((blocks,), jnp.int32),
            pltpu.VMEM(block_rows.shape, jnp.int32),
            pltpu.VMEM(block_slots.shape, jnp.int32),
            pltpu.SMEM((blocks,), jnp.int32),
            pltpu.SemaphoreType.DMA((5,)),
        ],
        name="plan",
    )(
        block_count,
        *(
            pltpu.with_memory_space_constraint(x, pltpu.HBM)
            for x in (block_table, block_peer[:, 0], block_len, block_rows, block_slots)
        )
    )


def fused_kernel(
    peers,
    near_blocks,
    index_ref,
    rows_ref,
    slots_ref,
    tables_hbm,
    in_ref,
    out_w_ref,
    mix_ref,
    bias_ref,
    gate_ref,
    result_ref,
    tables_ref,
    made_ref,
    first,
    held,
    emb,
    win,
    wout,
    table_sem,
    ring_send,
    ring_recv,
    w_send,
    w_recv,
    w_local,
):
    table_count, rows_dev, width = tables_ref.shape
    blocks, block = rows_ref.shape
    samples = result_ref.shape[0]
    part = table_count // STREAMS
    experts = mix_ref.shape[0]
    pieces = 2 * experts
    me = lax.axis_index("mp")
    half = peers // 2
    at = jnp.where(lax.rem(me, 2) == 0, lax.div(me, 2), peers - 1 - lax.div(me, 2))
    d = lax.axis_index("dp")
    twin = d + 1 - 2 * lax.rem(d, 2)
    across = lax.rem(d + 2, 4)

    def member(position):
        position = lax.rem(position + 2 * peers, peers)
        return jnp.where(position < half, 2 * position, 2 * (peers - 1 - position) + 1)

    ahead, behind = member(at + 1), member(at - 1)

    table_copies = [
        pltpu.make_async_copy(tables_hbm.at[t], tables_ref.at[t], table_sem.at[t])
        for t in range(table_count)
    ]
    for copy in table_copies:
        copy.start()

    barrier = pltpu.get_barrier_semaphore()
    greet = [{"mp": ahead}, {"mp": behind}, {"dp": twin}, {"dp": across}]
    for target in greet:
        pl.semaphore_signal(barrier, inc=1, device_id=target, device_id_type=MESH)
    made_ref[blocks] = jnp.zeros((samples, width), jnp.float32)
    pl.semaphore_wait(barrier, len(greet))

    def piece_refs(q, owner):
        if q < experts:
            return in_ref.at[q], win.at[owner, q]
        return out_w_ref.at[q - experts], wout.at[owner, q - experts]

    def w_copy(kind, q):
        source, place = piece_refs(q, across if kind == 2 else d)
        return pltpu.make_async_remote_copy(
            src_ref=place if kind == 2 else source,
            dst_ref=place,
            send_sem=w_send.at[kind, q],
            recv_sem=w_recv.at[kind, q],
            device_id={"dp": across if kind == 0 else twin},
            device_id_type=MESH,
        )

    for q in range(pieces):
        w_copy(0, q).start()

    def ring_copy(stream, source, step):
        target = ahead if stream % 2 == 0 else behind
        return pltpu.make_async_remote_copy(
            src_ref=source,
            dst_ref=held.at[step, stream],
            send_sem=ring_send.at[stream, step],
            recv_sem=ring_recv.at[stream, step],
            device_id={"mp": target},
            device_id_type=MESH,
        )

    def own_tile(stream, distance, i):
        dest = member(at - distance if stream % 2 == 0 else at + distance)
        return made_ref[index_ref[2 * blocks + dest * table_count + stream * part + i]]

    fold = FOLD if rows_dev % (FOLD * 128) == 0 else 1
    depth_rows = rows_dev // fold
    lane = lax.broadcasted_iota(jnp.int32, (block, 128), 1)
    sample = lax.broadcasted_iota(jnp.int32, (samples, block), 0)

    def group(g, carry):
        made = []
        for u in range(UNROLL):
            b = g * UNROLL + u
            table = index_ref[b]
            column = jnp.broadcast_to(rows_ref[pl.ds(b, 1), :], (128, block)).T
            low = lax.rem(column, depth_rows)
            high = lax.div(column, depth_rows)
            pick = jnp.concatenate(
                [
                    jnp.where(low == lane + c * 128, 1.0, 0.0).astype(jnp.bfloat16)
                    for c in range(depth_rows // 128)
                ],
                axis=1,
            )
            side = jnp.concatenate(
                [tables_ref[table, j * depth_rows : (j + 1) * depth_rows, :] for j in range(fold)],
                axis=1,
            )
            wide = jnp.dot(pick, side, preferred_element_type=jnp.float32)
            picked = wide[:, :width]
            for j in range(1, fold):
                picked = jnp.where(high == j, wide[:, j * width : (j + 1) * width], picked)
            place = jnp.where(sample == slots_ref[pl.ds(b, 1), :], 1.0, 0.0)
            made.append(
                jnp.dot(
                    place.astype(jnp.bfloat16),
                    picked.astype(jnp.bfloat16),
                    preferred_element_type=jnp.float32,
                )
            )
        for u in range(UNROLL):
            b = g * UNROLL + u
            made_ref[b] = made[u] + made_ref[index_ref[blocks + b]]
        return carry

    for copy in table_copies:
        copy.wait()
    lax.fori_loop(0, near_blocks // UNROLL, group, 0)
    for stream in range(STREAMS):
        for i in range(part):
            first[stream, i] = own_tile(stream, 1, i).astype(jnp.bfloat16)
        ring_copy(stream, first.at[stream], 0).start()
    for q in range(pieces):
        w_copy(1, q).start()
    local = []
    for q in range(pieces):
        source, place = piece_refs(q, d)
        local.append(pltpu.make_async_copy(source, place, w_local.at[q]))
        local[-1].start()
    lax.fori_loop(near_blocks // UNROLL, blocks // UNROLL, group, 0)

    def hop(step, last):
        for stream in range(STREAMS):
            ring_copy(stream, held.at[step, stream], step).wait_recv()
            for i in range(part):
                total = held[step, stream, i].astype(jnp.float32) + own_tile(stream, step + 2, i)
                total = total.astype(jnp.bfloat16)
                if last:
                    column = (stream * part + i) * width
                    emb[:, column : column + width] = total
                else:
                    held[step, stream, i] = total
            if not last:
                ring_copy(stream, held.at[step, stream], step + 1).start()

    passed = 0
    for step in range(peers - 2):
        hop(step, False)
        if passed < pieces:
            w_copy(0, passed).wait_recv()
            w_copy(2, passed).start()
            passed += 1
    hop(peers - 2, True)
    for q in range(passed, pieces):
        w_copy(0, q).wait_recv()
        w_copy(2, q).start()
    for copy in local:
        copy.wait()

    owners = win.shape[0]
    depth = in_ref.shape[1]
    columns = out_w_ref.shape[2]
    gate = jax.nn.sigmoid(
        lax.dot_general(
            emb[...], gate_ref[...], (((1,), (1,)), ((), ())), preferred_element_type=jnp.float32
        )
    )
    mixed = []
    for e in range(experts):
        w_copy(1, e).wait_recv()
        w_copy(2, e).wait_recv()
        projected = jnp.zeros((samples, in_ref.shape[2]), jnp.float32)
        for o in range(owners):
            projected += jnp.dot(
                emb[:, o * depth : (o + 1) * depth], win[o, e], preferred_element_type=jnp.float32
            )
        hidden = jnp.tanh(projected).astype(jnp.bfloat16)
        mixed.append(
            jnp.tanh(
                jnp.dot(hidden, mix_ref[e], preferred_element_type=jnp.float32)
            ).astype(jnp.bfloat16)
        )
    for e in range(experts):
        w_copy(1, experts + e).wait_recv()
        w_copy(2, experts + e).wait_recv()
    for o in range(owners):
        span = slice(o * columns, (o + 1) * columns)
        weighted = jnp.zeros((samples, columns), jnp.float32)
        for e in range(experts):
            grown = jnp.dot(mixed[e], wout[o, e], preferred_element_type=jnp.float32)
            weighted += gate[:, e : e + 1] * (grown + bias_ref[e : e + 1, span])
        base = emb[:, span].astype(jnp.float32)
        result_ref[:, span] = (base + base * weighted).astype(jnp.bfloat16)

    for stream in range(STREAMS):
        ring_copy(stream, first.at[stream], 0).wait_send()

    def sent(step, carry):
        for stream in range(STREAMS):
            ring_copy(stream, held.at[step - 1, stream], step).wait_send()
        return carry

    lax.fori_loop(1, peers - 1, sent, 0)
    for kind in (0, 1, 2):
        for q in range(pieces):
            w_copy(kind, q).wait_send()


def fused(
    peers,
    groups,
    tables,
    block_rows,
    block_slots,
    block_table,
    block_peer,
    block_len,
    block_count,
    cross_in,
    cross_mix,
    cross_out,
    cross_bias,
    gate_weight,
):
    table_count, _, width = tables.shape
    blocks = block_rows.shape[0]
    experts = cross_in.shape[0]
    rows, slots, index = plan(
        peers, table_count, block_rows, block_slots, block_table, block_peer, block_len, block_count
    )
    near_blocks = min(blocks, -(-4 * blocks // peers // UNROLL) * UNROLL)
    part = table_count // STREAMS
    hbm = pl.BlockSpec(memory_space=pltpu.HBM)
    vmem = pl.BlockSpec(memory_space=pltpu.VMEM)
    smem = pl.BlockSpec(memory_space=pltpu.SMEM)
    far = [pltpu.with_memory_space_constraint(x, pltpu.HBM) for x in (tables, cross_in, cross_out)]
    return pl.pallas_call(
        functools.partial(fused_kernel, peers, near_blocks),
        out_shape=jax.ShapeDtypeStruct((B_DEV, table_count * width), jnp.bfloat16),
        in_specs=[smem, vmem, vmem, hbm, hbm, hbm, vmem, vmem, vmem],
        out_specs=vmem,
        scratch_shapes=[
            pltpu.VMEM(tables.shape, jnp.bfloat16),
            pltpu.VMEM((blocks + 1, B_DEV, width), jnp.float32),
            pltpu.VMEM((STREAMS, part, B_DEV, width), jnp.bfloat16),
            pltpu.VMEM((peers - 1, STREAMS, part, B_DEV, width), jnp.bfloat16),
            pltpu.VMEM((B_DEV, table_count * width), jnp.bfloat16),
            pltpu.VMEM((groups, *cross_in.shape), jnp.bfloat16),
            pltpu.VMEM((groups, *cross_out.shape), jnp.bfloat16),
            pltpu.SemaphoreType.DMA((table_count,)),
            pltpu.SemaphoreType.DMA((STREAMS, peers - 1)),
            pltpu.SemaphoreType.DMA((STREAMS, peers - 1)),
            pltpu.SemaphoreType.DMA((3, 2 * experts)),
            pltpu.SemaphoreType.DMA((3, 2 * experts)),
            pltpu.SemaphoreType.DMA((2 * experts,)),
        ],
        compiler_params=pltpu.CompilerParams(
            collective_id=0,
            has_side_effects=True,
            vmem_limit_bytes=FUSED_LIMIT,
        ),
        name="fused",
    )(index, rows, slots, *far, cross_mix, cross_bias, gate_weight)


def shared(peers, groups, cross_out):
    return groups == 4 and cross_out.shape[2] % 128 == 0 and peers <= 8


def cross(peers, groups, partial, cross_in, cross_mix, cross_out, cross_bias, gate_weight):
    tiles, samples, width = partial.shape
    table_count = tiles // peers
    cross_in = lax.all_gather(cross_in, "dp", axis=1, tiled=True)
    cross_out = lax.all_gather(cross_out, "dp", axis=2, tiled=True)
    vmem = pl.BlockSpec(memory_space=pltpu.VMEM)
    return pl.pallas_call(
        functools.partial(cross_kernel, peers),
        out_shape=jax.ShapeDtypeStruct((samples, table_count * width), jnp.bfloat16),
        in_specs=[vmem] * 6,
        out_specs=vmem,
        scratch_shapes=[
            pltpu.VMEM((peers - 1, STREAMS, table_count // STREAMS, samples, width), jnp.bfloat16),
            pltpu.VMEM((samples, table_count * width), jnp.bfloat16),
            pltpu.SemaphoreType.DMA((STREAMS, peers - 1)),
            pltpu.SemaphoreType.DMA((STREAMS, peers - 1)),
        ],
        compiler_params=pltpu.CompilerParams(
            collective_id=0,
            has_side_effects=True,
            vmem_limit_bytes=VMEM_LIMIT,
        ),
        name="cross",
    )(partial, cross_in, cross_mix, cross_out, cross_bias, gate_weight)


def on_device(
    tables,
    block_rows,
    block_slots,
    block_table,
    block_peer,
    block_len,
    block_count,
    cross_in,
    cross_mix,
    cross_out,
    cross_bias,
    gate_weight,
):
    peers, groups = lax.axis_size("mp"), lax.axis_size("dp")
    if shared(peers, groups, cross_out) and block_rows.shape[0] % UNROLL == 0:
        return fused(
            peers,
            groups,
            tables,
            block_rows,
            block_slots,
            block_table,
            block_peer,
            block_len,
            block_count,
            cross_in,
            cross_mix,
            cross_out,
            cross_bias,
            gate_weight,
        )
    partial = pool(
        peers, tables, block_rows, block_slots, block_table, block_peer, block_len, block_count
    )
    return cross(
        peers, groups, partial, cross_in, cross_mix, cross_out, cross_bias, gate_weight
    )


def solution(mesh):
    in_specs = (
        P(None, "mp", None),
        P(("mp", "dp"), None),
        P(("mp", "dp"), None),
        P(("mp", "dp")),
        P(("mp", "dp"), None),
        P(("mp", "dp")),
        P(("mp", "dp")),
        P(None, "dp", None),
        P(),
        P(None, None, "dp"),
        P(),
        P(),
    )
    out_specs = P(("mp", "dp"), None)
    return jax.shard_map(
        on_device, mesh=mesh, in_specs=in_specs, out_specs=out_specs, check_vma=False
    )
```

```python
import functools

import jax
import jax.numpy as jnp
from jax import lax
from jax.experimental import pallas as pl
from jax.experimental.pallas import tpu as pltpu
from jax.sharding import PartitionSpec as P

B_DEV = 128
UNROLL = 8
STREAMS = 4
MESH = pl.DeviceIdType.MESH
POOL_LIMIT = 30 << 20
FUSED_LIMIT = 48 << 20
FOLD = 4
VMEM_LIMIT = 67043328


def pool_kernel(
    unroll,
    count_ref,
    table_hbm,
    peer_hbm,
    len_hbm,
    rows_hbm,
    slots_hbm,
    tables_hbm,
    out_ref,
    table_ref,
    peer_ref,
    len_ref,
    rows_ref,
    slots_ref,
    tables_ref,
    acc,
    slot_of,
    key_of,
    ready,
    small_sem,
    table_sem,
):
    table_count, rows_dev, width = tables_ref.shape
    total_blocks, block = rows_ref.shape
    tiles, samples, _ = out_ref.shape
    pairs = (
        (table_hbm, table_ref),
        (peer_hbm, peer_ref),
        (len_hbm, len_ref),
        (rows_hbm, rows_ref),
        (slots_hbm, slots_ref),
    )
    small = [pltpu.make_async_copy(a, b, small_sem.at[i]) for i, (a, b) in enumerate(pairs)]
    for copy in small:
        copy.start()

    def table_copy(t):
        return pltpu.make_async_copy(tables_hbm.at[t], tables_ref.at[t], table_sem.at[t])

    for t in range(table_count):
        table_copy(t).start()
        ready[t] = 0

    def need(t):
        @pl.when(ready[t] == 0)
        def _():
            table_copy(t).wait()
            ready[t] = 1

    def clear(i, carry):
        out_ref[i] = jnp.zeros((samples, width), jnp.bfloat16)
        slot_of[i] = -1
        return carry

    lax.fori_loop(0, tiles, clear, 0)
    for copy in small:
        copy.wait()
    count = count_ref[0]

    lane = lax.broadcasted_iota(jnp.int32, (block, 128), 1)
    sample = lax.broadcasted_iota(jnp.int32, (samples, block), 0)
    entry = lax.broadcasted_iota(jnp.int32, (samples, block), 1)

    def group(g, used):
        made = []
        for u in range(unroll):
            need(table_ref[g * unroll + u])
        for u in range(unroll):
            b = g * unroll + u
            row = rows_ref[pl.ds(b, 1), :]
            slot = slots_ref[pl.ds(b, 1), :]
            table = table_ref[b]
            column = jnp.broadcast_to(row, (128, block)).T
            pick = jnp.concatenate(
                [
                    jnp.where(column == lane + c * 128, 1.0, 0.0).astype(jnp.bfloat16)
                    for c in range(rows_dev // 128)
                ],
                axis=1,
            )
            picked = jnp.dot(pick, tables_ref[table], preferred_element_type=jnp.float32)
            place = jnp.where((sample == slot) & (entry < len_ref[b]), 1.0, 0.0)
            made.append(
                jnp.dot(
                    place.astype(jnp.bfloat16),
                    picked.astype(jnp.bfloat16),
                    preferred_element_type=jnp.float32,
                )
            )
        for u in range(unroll):
            b = g * unroll + u
            key = peer_ref[b] * table_count + table_ref[b]
            live = b < count
            known = slot_of[key]
            first = known < 0
            at = jnp.where(live, jnp.where(first, used, known), total_blocks)
            acc[at] = jnp.where(first, made[u], acc[at] + made[u])
            slot_of[key] = jnp.where(live, at, known)
            key_of[at] = key
            used = used + jnp.where(live & first, 1, 0)
        return used

    used = lax.fori_loop(0, (count + unroll - 1) // unroll, group, 0)

    def flush(i, carry):
        out_ref[key_of[i]] = acc[i].astype(jnp.bfloat16)
        return carry

    lax.fori_loop(0, used, flush, 0)
    for t in range(table_count):
        need(t)


def pool(peers, tables, block_rows, block_slots, block_table, block_peer, block_len, block_count):
    table_count, _, width = tables.shape
    total_blocks = block_rows.shape[0]
    tiles = peers * table_count
    unroll = UNROLL if total_blocks % UNROLL == 0 else 1
    hbm = pl.BlockSpec(memory_space=pltpu.HBM)
    vmem = pl.BlockSpec(memory_space=pltpu.VMEM)
    return pl.pallas_call(
        functools.partial(pool_kernel, unroll),
        out_shape=jax.ShapeDtypeStruct((tiles, B_DEV, width), jnp.bfloat16),
        in_specs=[pl.BlockSpec(memory_space=pltpu.SMEM)] + [hbm] * 6,
        out_specs=vmem,
        scratch_shapes=[
            pltpu.SMEM((total_blocks,), jnp.int32),
            pltpu.SMEM((total_blocks,), jnp.int32),
            pltpu.SMEM((total_blocks,), jnp.int32),
            pltpu.VMEM(block_rows.shape, jnp.int32),
            pltpu.VMEM(block_slots.shape, jnp.int32),
            pltpu.VMEM(tables.shape, jnp.bfloat16),
            pltpu.VMEM((total_blocks + 1, B_DEV, width), jnp.float32),
            pltpu.SMEM((tiles,), jnp.int32),
            pltpu.SMEM((total_blocks + 1,), jnp.int32),
            pltpu.SMEM((table_count,), jnp.int32),
            pltpu.SemaphoreType.DMA((5,)),
            pltpu.SemaphoreType.DMA((table_count,)),
        ],
        compiler_params=pltpu.CompilerParams(
            vmem_limit_bytes=POOL_LIMIT if peers <= 8 else VMEM_LIMIT
        ),
        cost_estimate=pl.CostEstimate(
            flops=2 * total_blocks * B_DEV * tables.shape[1] * width,
            bytes_accessed=2 * tables.size + 2 * tiles * B_DEV * width,
            transcendentals=0,
        ),
        name="pool",
    )(
        block_count,
        *(
            pltpu.with_memory_space_constraint(x, pltpu.HBM)
            for x in (
                block_table,
                block_peer[:, 0],
                block_len,
                block_rows,
                block_slots,
                tables,
            )
        )
    )


def cross_kernel(
    peers,
    partial_ref,
    in_ref,
    mix_ref,
    out_w_ref,
    bias_ref,
    gate_ref,
    result_ref,
    held,
    emb,
    ring_send,
    ring_recv,
):
    tiles, samples, width = partial_ref.shape
    table_count = tiles // peers
    part = table_count // STREAMS
    experts = mix_ref.shape[0]
    me = lax.axis_index("mp")
    half = peers // 2
    at = jnp.where(lax.rem(me, 2) == 0, lax.div(me, 2), peers - 1 - lax.div(me, 2))

    def member(position):
        position = lax.rem(position + 2 * peers, peers)
        return jnp.where(position < half, 2 * position, 2 * (peers - 1 - position) + 1)

    ahead, behind = member(at + 1), member(at - 1)

    barrier = pltpu.get_barrier_semaphore()
    greet = [{"mp": ahead}, {"mp": behind}]
    for target in greet:
        pl.semaphore_signal(barrier, inc=1, device_id=target, device_id_type=MESH)
    pl.semaphore_wait(barrier, len(greet))

    def ring_copy(stream, source, step):
        target = ahead if stream % 2 == 0 else behind
        return pltpu.make_async_remote_copy(
            src_ref=source,
            dst_ref=held.at[step, stream],
            send_sem=ring_send.at[stream, step],
            recv_sem=ring_recv.at[stream, step],
            device_id={"mp": target},
            device_id_type=MESH,
        )

    def own_tiles(stream, distance):
        dest = member(at - distance if stream % 2 == 0 else at + distance)
        return pl.ds(dest * table_count + stream * part, part)

    for stream in range(STREAMS):
        ring_copy(stream, partial_ref.at[own_tiles(stream, 1)], 0).start()

    def hop(step, last):
        for stream in range(STREAMS):
            ring_copy(stream, held.at[step, stream], step).wait_recv()
            mine = partial_ref[own_tiles(stream, step + 2)]
            total = held[step, stream].astype(jnp.float32) + mine.astype(jnp.float32)
            total = total.astype(jnp.bfloat16)
            if last:
                for i in range(part):
                    column = (stream * part + i) * width
                    emb[:, column : column + width] = total[i]
            else:
                held[step, stream] = total
                ring_copy(stream, held.at[step, stream], step + 1).start()

    def turn(step, carry):
        hop(step, False)
        return carry

    lax.fori_loop(0, peers - 2, turn, 0)
    hop(peers - 2, True)

    gate = jax.nn.sigmoid(
        lax.dot_general(
            emb[...], gate_ref[...], (((1,), (1,)), ((), ())), preferred_element_type=jnp.float32
        )
    )
    mixed = []
    for e in range(experts):
        projected = jnp.dot(emb[...], in_ref[e], preferred_element_type=jnp.float32)
        hidden = jnp.tanh(projected).astype(jnp.bfloat16)
        mixed.append(
            jnp.tanh(
                jnp.dot(hidden, mix_ref[e], preferred_element_type=jnp.float32)
            ).astype(jnp.bfloat16)
        )
    weighted = jnp.zeros(emb.shape, jnp.float32)
    for e in range(experts):
        grown = jnp.dot(mixed[e], out_w_ref[e], preferred_element_type=jnp.float32)
        weighted += gate[:, e : e + 1] * (grown + bias_ref[e : e + 1, :])
    base = emb[...].astype(jnp.float32)
    result_ref[...] = (base + base * weighted).astype(jnp.bfloat16)

    for stream in range(STREAMS):
        ring_copy(stream, partial_ref.at[own_tiles(stream, 1)], 0).wait_send()

    def sent(step, carry):
        for stream in range(STREAMS):
            ring_copy(stream, held.at[step - 1, stream], step).wait_send()
        return carry

    lax.fori_loop(1, peers - 1, sent, 0)


def order_blocks(peers, part, at, count, table, peer, length, plan_ref):
    blocks = table.shape[1]
    table_count = STREAMS * part
    square = (blocks, blocks)
    across = lax.broadcasted_iota(jnp.int32, square, 1)
    down = lax.broadcasted_iota(jnp.int32, square, 0)

    def turned(row):
        return jnp.broadcast_to(row, square).T

    def total(x):
        return jnp.sum(x, axis=0, keepdims=True)

    number = lax.broadcasted_iota(jnp.int32, (1, blocks), 1)
    live = number < count
    half = lax.shift_right_logical(peer, 1)
    place = jnp.where((peer & 1) == 0, half, peers - 1 - half)
    forward = table < part
    for stream in range(2, STREAMS, 2):
        forward = forward | ((table >= stream * part) & (table < (stream + 1) * part))
    away = jnp.where(forward, at - place, place - at)
    near = jnp.where(live & ((away == 1) | (away == 1 - peers)), 1, 0)
    key = jnp.where(live, peer * table_count + table, -1)
    near_down = turned(near)
    before = down < across
    near_rank = total(jnp.where(before, near_down, 0))
    far_rank = total(jnp.where(before, 1 - near_down, 0))
    found = total(near_down)
    spot = jnp.where(near == 1, near_rank, found + far_rank)
    chosen = turned(spot) == across
    ordered_key = total(jnp.where(chosen, turned(key), 0))
    ordered_down = turned(ordered_key)
    known = jnp.where((ordered_down == ordered_key) & before, down, -1)
    known = jnp.max(known, axis=0, keepdims=True)
    tiles = peers * table_count
    wanted = lax.broadcasted_iota(jnp.int32, (blocks, tiles), 1)
    ordinal = lax.broadcasted_iota(jnp.int32, (blocks, tiles), 0)
    key_down = jnp.broadcast_to(ordered_down[:, :1], (blocks, tiles))
    latest = jnp.max(jnp.where(key_down == wanted, ordinal, -1), axis=0, keepdims=True)
    plan_ref[0:1, :blocks] = total(jnp.where(chosen, down, 0))
    plan_ref[1:2, :blocks] = total(jnp.where(chosen, turned(table), 0))
    plan_ref[2:3, :blocks] = total(jnp.where(chosen, turned(jnp.where(live, length, 0)), 0))
    plan_ref[3:4, :blocks] = jnp.where(known < 0, blocks, known)
    plan_ref[4:5, :tiles] = jnp.where(latest < 0, blocks, latest)


def fused_kernel(
    peers,
    near_blocks,
    count_ref,
    table_hbm,
    peer_hbm,
    len_hbm,
    rows_hbm,
    slots_hbm,
    tables_hbm,
    in_ref,
    out_w_ref,
    mix_hbm,
    bias_hbm,
    gate_hbm,
    result_ref,
    table_row,
    peer_row,
    len_row,
    rows_ref,
    slots_ref,
    mix_ref,
    bias_ref,
    gate_ref,
    plan_ref,
    index_ref,
    tables_ref,
    made_ref,
    first,
    held,
    emb,
    win,
    wout,
    small_sem,
    table_sem,
    ring_send,
    ring_recv,
    w_send,
    w_recv,
    w_local,
):
    table_count, rows_dev, width = tables_ref.shape
    blocks, block = rows_ref.shape
    samples = result_ref.shape[0]
    part = table_count // STREAMS
    experts = mix_ref.shape[0]
    pieces = 2 * experts
    me = lax.axis_index("mp")
    half = peers // 2
    at = jnp.where(lax.rem(me, 2) == 0, lax.div(me, 2), peers - 1 - lax.div(me, 2))
    d = lax.axis_index("dp")
    twin = d + 1 - 2 * lax.rem(d, 2)
    across = lax.rem(d + 2, 4)

    def member(position):
        position = lax.rem(position + 2 * peers, peers)
        return jnp.where(position < half, 2 * position, 2 * (peers - 1 - position) + 1)

    ahead, behind = member(at + 1), member(at - 1)

    pairs = (
        (table_hbm, table_row),
        (peer_hbm, peer_row),
        (len_hbm, len_row),
        (rows_hbm, rows_ref),
        (slots_hbm, slots_ref),
        (mix_hbm, mix_ref),
        (bias_hbm, bias_ref),
        (gate_hbm, gate_ref),
        (plan_ref, index_ref),
    )
    small = [pltpu.make_async_copy(a, b, small_sem.at[i]) for i, (a, b) in enumerate(pairs)]
    for copy in small[:5]:
        copy.start()
    table_copies = [
        pltpu.make_async_copy(tables_hbm.at[t], tables_ref.at[t], table_sem.at[t])
        for t in range(table_count)
    ]
    for copy in table_copies:
        copy.start()
    for copy in small[5:8]:
        copy.start()

    barrier = pltpu.get_barrier_semaphore()
    greet = [{"mp": ahead}, {"mp": behind}, {"dp": twin}, {"dp": across}]
    for target in greet:
        pl.semaphore_signal(barrier, inc=1, device_id=target, device_id_type=MESH)
    made_ref[blocks] = jnp.zeros((samples, width), jnp.float32)
    pl.semaphore_wait(barrier, len(greet))

    def piece_refs(q, owner):
        if q < experts:
            return in_ref.at[q], win.at[owner, q]
        return out_w_ref.at[q - experts], wout.at[owner, q - experts]

    def w_copy(kind, q):
        source, place = piece_refs(q, across if kind == 2 else d)
        return pltpu.make_async_remote_copy(
            src_ref=place if kind == 2 else source,
            dst_ref=place,
            send_sem=w_send.at[kind, q],
            recv_sem=w_recv.at[kind, q],
            device_id={"dp": across if kind == 0 else twin},
            device_id_type=MESH,
        )

    for q in range(pieces):
        w_copy(0, q).start()

    for copy in small[:5]:
        copy.wait()
    order_blocks(peers, part, at, count_ref[0], table_row[...], peer_row[...], len_row[...], plan_ref)
    small[8].start()

    def ring_copy(stream, source, step):
        target = ahead if stream % 2 == 0 else behind
        return pltpu.make_async_remote_copy(
            src_ref=source,
            dst_ref=held.at[step, stream],
            send_sem=ring_send.at[stream, step],
            recv_sem=ring_recv.at[stream, step],
            device_id={"mp": target},
            device_id_type=MESH,
        )

    def own_tile(stream, distance, i):
        dest = member(at - distance if stream % 2 == 0 else at + distance)
        return made_ref[index_ref[4, dest * table_count + stream * part + i]]

    even = rows_dev & (rows_dev - 1) == 0 and rows_dev >= FOLD * 128
    fold = FOLD if even else 1
    depth_rows = rows_dev // fold
    lane = lax.broadcasted_iota(jnp.int32, (block, 128), 1)
    sample = lax.broadcasted_iota(jnp.int32, (samples, block), 0)
    entry = lax.broadcasted_iota(jnp.int32, (samples, block), 1)

    def group(g, carry):
        made = []
        for u in range(UNROLL):
            b = g * UNROLL + u
            source = index_ref[0, b]
            table = index_ref[1, b]
            column = jnp.broadcast_to(rows_ref[pl.ds(source, 1), :], (128, block)).T
            low = column & (depth_rows - 1) if even else column
            high = lax.shift_right_logical(column, depth_rows.bit_length() - 1)
            pick = jnp.concatenate(
                [
                    jnp.where(low == lane + c * 128, 1.0, 0.0).astype(jnp.bfloat16)
                    for c in range(depth_rows // 128)
                ],
                axis=1,
            )
            side = jnp.concatenate(
                [tables_ref[table, j * depth_rows : (j + 1) * depth_rows, :] for j in range(fold)],
                axis=1,
            )
            wide = jnp.dot(pick, side, preferred_element_type=jnp.float32)
            picked = wide[:, :width]
            for j in range(1, fold):
                picked = jnp.where(high == j, wide[:, j * width : (j + 1) * width], picked)
            slot = slots_ref[pl.ds(source, 1), :]
            place = jnp.where((sample == slot) & (entry < index_ref[2, b]), 1.0, 0.0)
            made.append(
                jnp.dot(
                    place.astype(jnp.bfloat16),
                    picked.astype(jnp.bfloat16),
                    preferred_element_type=jnp.float32,
                )
            )
        for u in range(UNROLL):
            b = g * UNROLL + u
            made_ref[b] = made[u] + made_ref[index_ref[3, b]]
        return carry

    small[8].wait()
    for copy in table_copies:
        copy.wait()
    lax.fori_loop(0, near_blocks // UNROLL, group, 0)
    for stream in range(STREAMS):
        for i in range(part):
            first[stream, i] = own_tile(stream, 1, i).astype(jnp.bfloat16)
        ring_copy(stream, first.at[stream], 0).start()
    for q in range(pieces):
        w_copy(1, q).start()
    local = []
    for q in range(pieces):
        source, place = piece_refs(q, d)
        local.append(pltpu.make_async_copy(source, place, w_local.at[q]))
        local[-1].start()
    lax.fori_loop(near_blocks // UNROLL, blocks // UNROLL, group, 0)

    span = part * width
    gated = [jnp.zeros((samples, experts), jnp.float32)]
    projected = [jnp.zeros((samples, in_ref.shape[2]), jnp.float32) for _ in range(experts)]

    def hop(step, last):
        for stream in range(STREAMS):
            ring_copy(stream, held.at[step, stream], step).wait_recv()
            for i in range(part):
                total = held[step, stream, i].astype(jnp.float32) + own_tile(stream, step + 2, i)
                total = total.astype(jnp.bfloat16)
                if last:
                    column = (stream * part + i) * width
                    emb[:, column : column + width] = total
                else:
                    held[step, stream, i] = total
            if not last:
                ring_copy(stream, held.at[step, stream], step + 1).start()
                continue
            columns = slice(stream * span, (stream + 1) * span)
            ready = emb[:, columns]
            gated[0] += lax.dot_general(
                ready,
                gate_ref[:, columns],
                (((1,), (1,)), ((), ())),
                preferred_element_type=jnp.float32,
            )
            for e in range(experts):
                projected[e] += jnp.dot(ready, win[stream, e], preferred_element_type=jnp.float32)

    def forward(first_piece, end_piece):
        for q in range(first_piece, end_piece):
            w_copy(0, q).wait_recv()
            w_copy(2, q).start()

    for step in range(peers - 2):
        hop(step, False)
        forward(min(step, pieces - 1), min(step + 1, pieces - 1))
    forward(min(peers - 2, pieces - 1), pieces - 1)
    for copy in local:
        copy.wait()
    for copy in small[5:8]:
        copy.wait()
    for e in range(experts):
        w_copy(1, e).wait_recv()
        w_copy(2, e).wait_recv()
    hop(peers - 2, True)
    forward(pieces - 1, pieces)

    owners = win.shape[0]
    columns = out_w_ref.shape[2]
    gate = jax.nn.sigmoid(gated[0])
    mixed = []
    for e in range(experts):
        hidden = jnp.tanh(projected[e]).astype(jnp.bfloat16)
        mixed.append(
            jnp.tanh(
                jnp.dot(hidden, mix_ref[e], preferred_element_type=jnp.float32)
            ).astype(jnp.bfloat16)
        )
    for e in range(experts):
        w_copy(1, experts + e).wait_recv()
        w_copy(2, experts + e).wait_recv()
    for o in range(owners):
        span = slice(o * columns, (o + 1) * columns)
        weighted = jnp.zeros((samples, columns), jnp.float32)
        for e in range(experts):
            grown = jnp.dot(mixed[e], wout[o, e], preferred_element_type=jnp.float32)
            weighted += gate[:, e : e + 1] * (grown + bias_ref[e : e + 1, span])
        base = emb[:, span].astype(jnp.float32)
        result_ref[:, span] = (base + base * weighted).astype(jnp.bfloat16)

    for stream in range(STREAMS):
        ring_copy(stream, first.at[stream], 0).wait_send()

    def sent(step, carry):
        for stream in range(STREAMS):
            ring_copy(stream, held.at[step - 1, stream], step).wait_send()
        return carry

    lax.fori_loop(1, peers - 1, sent, 0)
    for kind in (0, 1, 2):
        for q in range(pieces):
            w_copy(kind, q).wait_send()


def fused(
    peers,
    groups,
    tables,
    block_rows,
    block_slots,
    block_table,
    block_peer,
    block_len,
    block_count,
    cross_in,
    cross_mix,
    cross_out,
    cross_bias,
    gate_weight,
):
    table_count, _, width = tables.shape
    blocks = block_rows.shape[0]
    experts = cross_in.shape[0]
    near_blocks = min(blocks, -(-4 * blocks // peers // UNROLL) * UNROLL)
    part = table_count // STREAMS
    hbm = pl.BlockSpec(memory_space=pltpu.HBM)
    vmem = pl.BlockSpec(memory_space=pltpu.VMEM)
    lanes = -(-max(blocks, peers * table_count) // 128) * 128
    operands = (
        block_table.reshape(1, blocks),
        block_peer.reshape(1, blocks),
        block_len.reshape(1, blocks),
        block_rows,
        block_slots,
        tables,
        cross_in,
        cross_out,
        cross_mix,
        cross_bias,
        gate_weight,
    )
    return pl.pallas_call(
        functools.partial(fused_kernel, peers, near_blocks),
        out_shape=jax.ShapeDtypeStruct((B_DEV, table_count * width), jnp.bfloat16),
        in_specs=[pl.BlockSpec(memory_space=pltpu.SMEM)] + [hbm] * len(operands),
        out_specs=vmem,
        scratch_shapes=[
            pltpu.VMEM((1, blocks), jnp.int32),
            pltpu.VMEM((1, blocks), jnp.int32),
            pltpu.VMEM((1, blocks), jnp.int32),
            pltpu.VMEM(block_rows.shape, jnp.int32),
            pltpu.VMEM(block_slots.shape, jnp.int32),
            pltpu.VMEM(cross_mix.shape, jnp.bfloat16),
            pltpu.VMEM(cross_bias.shape, jnp.float32),
            pltpu.VMEM(gate_weight.shape, jnp.bfloat16),
            pltpu.VMEM((8, lanes), jnp.int32),
            pltpu.SMEM((8, lanes), jnp.int32),
            pltpu.VMEM(tables.shape, jnp.bfloat16),
            pltpu.VMEM((blocks + 1, B_DEV, width), jnp.float32),
            pltpu.VMEM((STREAMS, part, B_DEV, width), jnp.bfloat16),
            pltpu.VMEM((peers - 1, STREAMS, part, B_DEV, width), jnp.bfloat16),
            pltpu.VMEM((B_DEV, table_count * width), jnp.bfloat16),
            pltpu.VMEM((groups, *cross_in.shape), jnp.bfloat16),
            pltpu.VMEM((groups, *cross_out.shape), jnp.bfloat16),
            pltpu.SemaphoreType.DMA((9,)),
            pltpu.SemaphoreType.DMA((table_count,)),
            pltpu.SemaphoreType.DMA((STREAMS, peers - 1)),
            pltpu.SemaphoreType.DMA((STREAMS, peers - 1)),
            pltpu.SemaphoreType.DMA((3, 2 * experts)),
            pltpu.SemaphoreType.DMA((3, 2 * experts)),
            pltpu.SemaphoreType.DMA((2 * experts,)),
        ],
        compiler_params=pltpu.CompilerParams(
            collective_id=0,
            has_side_effects=True,
            vmem_limit_bytes=FUSED_LIMIT,
        ),
        name="fused",
    )(block_count, *(pltpu.with_memory_space_constraint(x, pltpu.HBM) for x in operands))


def shared(peers, groups, cross_out):
    return groups == 4 and cross_out.shape[2] % 128 == 0 and peers <= 8


def cross(peers, groups, partial, cross_in, cross_mix, cross_out, cross_bias, gate_weight):
    tiles, samples, width = partial.shape
    table_count = tiles // peers
    cross_in = lax.all_gather(cross_in, "dp", axis=1, tiled=True)
    cross_out = lax.all_gather(cross_out, "dp", axis=2, tiled=True)
    vmem = pl.BlockSpec(memory_space=pltpu.VMEM)
    return pl.pallas_call(
        functools.partial(cross_kernel, peers),
        out_shape=jax.ShapeDtypeStruct((samples, table_count * width), jnp.bfloat16),
        in_specs=[vmem] * 6,
        out_specs=vmem,
        scratch_shapes=[
            pltpu.VMEM((peers - 1, STREAMS, table_count // STREAMS, samples, width), jnp.bfloat16),
            pltpu.VMEM((samples, table_count * width), jnp.bfloat16),
            pltpu.SemaphoreType.DMA((STREAMS, peers - 1)),
            pltpu.SemaphoreType.DMA((STREAMS, peers - 1)),
        ],
        compiler_params=pltpu.CompilerParams(
            collective_id=0,
            has_side_effects=True,
            vmem_limit_bytes=VMEM_LIMIT,
        ),
        name="cross",
    )(partial, cross_in, cross_mix, cross_out, cross_bias, gate_weight)


def on_device(
    tables,
    block_rows,
    block_slots,
    block_table,
    block_peer,
    block_len,
    block_count,
    cross_in,
    cross_mix,
    cross_out,
    cross_bias,
    gate_weight,
):
    peers, groups = lax.axis_size("mp"), lax.axis_size("dp")
    if shared(peers, groups, cross_out) and block_rows.shape[0] % UNROLL == 0:
        return fused(
            peers,
            groups,
            tables,
            block_rows,
            block_slots,
            block_table,
            block_peer,
            block_len,
            block_count,
            cross_in,
            cross_mix,
            cross_out,
            cross_bias,
            gate_weight,
        )
    partial = pool(
        peers, tables, block_rows, block_slots, block_table, block_peer, block_len, block_count
    )
    return cross(
        peers, groups, partial, cross_in, cross_mix, cross_out, cross_bias, gate_weight
    )


def solution(mesh):
    in_specs = (
        P(None, "mp", None),
        P(("mp", "dp"), None),
        P(("mp", "dp"), None),
        P(("mp", "dp")),
        P(("mp", "dp"), None),
        P(("mp", "dp")),
        P(("mp", "dp")),
        P(None, "dp", None),
        P(),
        P(None, None, "dp"),
        P(),
        P(),
    )
    out_specs = P(("mp", "dp"), None)
    return jax.shard_map(
        on_device, mesh=mesh, in_specs=in_specs, out_specs=out_specs, check_vma=False
    )
```

```python
import functools

import jax
import jax.numpy as jnp
from jax import lax
from jax.experimental import pallas as pl
from jax.experimental.pallas import tpu as pltpu
from jax.sharding import PartitionSpec as P

B_DEV = 128
UNROLL = 8
STREAMS = 4
MESH = pl.DeviceIdType.MESH
POOL_LIMIT = 30 << 20
FUSED_LIMIT = 48 << 20
FOLD = 4
RING = 4
GROUP = 16
SHARE = 320
VMEM_LIMIT = 67043328


def pool_kernel(
    unroll,
    count_ref,
    table_hbm,
    peer_hbm,
    len_hbm,
    rows_hbm,
    slots_hbm,
    tables_hbm,
    out_ref,
    table_ref,
    peer_ref,
    len_ref,
    rows_ref,
    slots_ref,
    tables_ref,
    acc,
    slot_of,
    key_of,
    ready,
    small_sem,
    table_sem,
):
    table_count, rows_dev, width = tables_ref.shape
    total_blocks, block = rows_ref.shape
    tiles, samples, _ = out_ref.shape
    pairs = (
        (table_hbm, table_ref),
        (peer_hbm, peer_ref),
        (len_hbm, len_ref),
        (rows_hbm, rows_ref),
        (slots_hbm, slots_ref),
    )
    small = [pltpu.make_async_copy(a, b, small_sem.at[i]) for i, (a, b) in enumerate(pairs)]
    for copy in small:
        copy.start()

    def table_copy(t):
        return pltpu.make_async_copy(tables_hbm.at[t], tables_ref.at[t], table_sem.at[t])

    for t in range(table_count):
        table_copy(t).start()
        ready[t] = 0

    def need(t):
        @pl.when(ready[t] == 0)
        def _():
            table_copy(t).wait()
            ready[t] = 1

    def clear(i, carry):
        out_ref[i] = jnp.zeros((samples, width), jnp.bfloat16)
        slot_of[i] = -1
        return carry

    lax.fori_loop(0, tiles, clear, 0)
    for copy in small:
        copy.wait()
    count = count_ref[0]

    lane = lax.broadcasted_iota(jnp.int32, (block, 128), 1)
    sample = lax.broadcasted_iota(jnp.int32, (samples, block), 0)
    entry = lax.broadcasted_iota(jnp.int32, (samples, block), 1)

    def group(g, used):
        made = []
        for u in range(unroll):
            need(table_ref[g * unroll + u])
        for u in range(unroll):
            b = g * unroll + u
            row = rows_ref[pl.ds(b, 1), :]
            slot = slots_ref[pl.ds(b, 1), :]
            table = table_ref[b]
            column = jnp.broadcast_to(row, (128, block)).T
            pick = jnp.concatenate(
                [
                    jnp.where(column == lane + c * 128, 1.0, 0.0).astype(jnp.bfloat16)
                    for c in range(rows_dev // 128)
                ],
                axis=1,
            )
            picked = jnp.dot(pick, tables_ref[table], preferred_element_type=jnp.float32)
            place = jnp.where((sample == slot) & (entry < len_ref[b]), 1.0, 0.0)
            made.append(
                jnp.dot(
                    place.astype(jnp.bfloat16),
                    picked.astype(jnp.bfloat16),
                    preferred_element_type=jnp.float32,
                )
            )
        for u in range(unroll):
            b = g * unroll + u
            key = peer_ref[b] * table_count + table_ref[b]
            live = b < count
            known = slot_of[key]
            first = known < 0
            at = jnp.where(live, jnp.where(first, used, known), total_blocks)
            acc[at] = jnp.where(first, made[u], acc[at] + made[u])
            slot_of[key] = jnp.where(live, at, known)
            key_of[at] = key
            used = used + jnp.where(live & first, 1, 0)
        return used

    used = lax.fori_loop(0, (count + unroll - 1) // unroll, group, 0)

    def flush(i, carry):
        out_ref[key_of[i]] = acc[i].astype(jnp.bfloat16)
        return carry

    lax.fori_loop(0, used, flush, 0)
    for t in range(table_count):
        need(t)


def pool(peers, tables, block_rows, block_slots, block_table, block_peer, block_len, block_count):
    table_count, _, width = tables.shape
    total_blocks = block_rows.shape[0]
    tiles = peers * table_count
    unroll = UNROLL if total_blocks % UNROLL == 0 else 1
    hbm = pl.BlockSpec(memory_space=pltpu.HBM)
    vmem = pl.BlockSpec(memory_space=pltpu.VMEM)
    return pl.pallas_call(
        functools.partial(pool_kernel, unroll),
        out_shape=jax.ShapeDtypeStruct((tiles, B_DEV, width), jnp.bfloat16),
        in_specs=[pl.BlockSpec(memory_space=pltpu.SMEM)] + [hbm] * 6,
        out_specs=vmem,
        scratch_shapes=[
            pltpu.SMEM((total_blocks,), jnp.int32),
            pltpu.SMEM((total_blocks,), jnp.int32),
            pltpu.SMEM((total_blocks,), jnp.int32),
            pltpu.VMEM(block_rows.shape, jnp.int32),
            pltpu.VMEM(block_slots.shape, jnp.int32),
            pltpu.VMEM(tables.shape, jnp.bfloat16),
            pltpu.VMEM((total_blocks + 1, B_DEV, width), jnp.float32),
            pltpu.SMEM((tiles,), jnp.int32),
            pltpu.SMEM((total_blocks + 1,), jnp.int32),
            pltpu.SMEM((table_count,), jnp.int32),
            pltpu.SemaphoreType.DMA((5,)),
            pltpu.SemaphoreType.DMA((table_count,)),
        ],
        compiler_params=pltpu.CompilerParams(
            vmem_limit_bytes=POOL_LIMIT if peers <= 8 else VMEM_LIMIT
        ),
        cost_estimate=pl.CostEstimate(
            flops=2 * total_blocks * B_DEV * tables.shape[1] * width,
            bytes_accessed=2 * tables.size + 2 * tiles * B_DEV * width,
            transcendentals=0,
        ),
        name="pool",
    )(
        block_count,
        *(
            pltpu.with_memory_space_constraint(x, pltpu.HBM)
            for x in (
                block_table,
                block_peer[:, 0],
                block_len,
                block_rows,
                block_slots,
                tables,
            )
        )
    )


def cross_kernel(
    peers,
    partial_ref,
    in_ref,
    mix_ref,
    out_w_ref,
    bias_ref,
    gate_ref,
    result_ref,
    held,
    emb,
    ring_send,
    ring_recv,
):
    tiles, samples, width = partial_ref.shape
    table_count = tiles // peers
    part = table_count // STREAMS
    experts = mix_ref.shape[0]
    me = lax.axis_index("mp")
    half = peers // 2
    at = jnp.where(lax.rem(me, 2) == 0, lax.div(me, 2), peers - 1 - lax.div(me, 2))

    def member(position):
        position = lax.rem(position + 2 * peers, peers)
        return jnp.where(position < half, 2 * position, 2 * (peers - 1 - position) + 1)

    ahead, behind = member(at + 1), member(at - 1)

    barrier = pltpu.get_barrier_semaphore()
    greet = [{"mp": ahead}, {"mp": behind}]
    for target in greet:
        pl.semaphore_signal(barrier, inc=1, device_id=target, device_id_type=MESH)
    pl.semaphore_wait(barrier, len(greet))

    def ring_copy(stream, source, step):
        target = ahead if stream % 2 == 0 else behind
        return pltpu.make_async_remote_copy(
            src_ref=source,
            dst_ref=held.at[step, stream],
            send_sem=ring_send.at[stream, step],
            recv_sem=ring_recv.at[stream, step],
            device_id={"mp": target},
            device_id_type=MESH,
        )

    def own_tiles(stream, distance):
        dest = member(at - distance if stream % 2 == 0 else at + distance)
        return pl.ds(dest * table_count + stream * part, part)

    for stream in range(STREAMS):
        ring_copy(stream, partial_ref.at[own_tiles(stream, 1)], 0).start()

    def hop(step, last):
        for stream in range(STREAMS):
            ring_copy(stream, held.at[step, stream], step).wait_recv()
            mine = partial_ref[own_tiles(stream, step + 2)]
            total = held[step, stream].astype(jnp.float32) + mine.astype(jnp.float32)
            total = total.astype(jnp.bfloat16)
            if last:
                for i in range(part):
                    column = (stream * part + i) * width
                    emb[:, column : column + width] = total[i]
            else:
                held[step, stream] = total
                ring_copy(stream, held.at[step, stream], step + 1).start()

    def turn(step, carry):
        hop(step, False)
        return carry

    lax.fori_loop(0, peers - 2, turn, 0)
    hop(peers - 2, True)

    gate = jax.nn.sigmoid(
        lax.dot_general(
            emb[...], gate_ref[...], (((1,), (1,)), ((), ())), preferred_element_type=jnp.float32
        )
    )
    mixed = []
    for e in range(experts):
        projected = jnp.dot(emb[...], in_ref[e], preferred_element_type=jnp.float32)
        hidden = jnp.tanh(projected).astype(jnp.bfloat16)
        mixed.append(
            jnp.tanh(
                jnp.dot(hidden, mix_ref[e], preferred_element_type=jnp.float32)
            ).astype(jnp.bfloat16)
        )
    weighted = jnp.zeros(emb.shape, jnp.float32)
    for e in range(experts):
        grown = jnp.dot(mixed[e], out_w_ref[e], preferred_element_type=jnp.float32)
        weighted += gate[:, e : e + 1] * (grown + bias_ref[e : e + 1, :])
    base = emb[...].astype(jnp.float32)
    result_ref[...] = (base + base * weighted).astype(jnp.bfloat16)

    for stream in range(STREAMS):
        ring_copy(stream, partial_ref.at[own_tiles(stream, 1)], 0).wait_send()

    def sent(step, carry):
        for stream in range(STREAMS):
            ring_copy(stream, held.at[step - 1, stream], step).wait_send()
        return carry

    lax.fori_loop(1, peers - 1, sent, 0)


def order_blocks(peers, table_count, cap, first_ahead, at, count, table, peer, length, plan_ref):
    blocks = table.shape[1]
    slots = blocks + cap
    number = lax.broadcasted_iota(jnp.int32, (1, blocks), 1)
    before = lax.broadcasted_iota(jnp.int32, (blocks, blocks), 0) < lax.broadcasted_iota(
        jnp.int32, (blocks, blocks), 1
    )

    def turned(row):
        size = row.shape[1]
        return jnp.broadcast_to(row, (size, size)).T

    def total(x):
        return jnp.sum(x, axis=0, keepdims=True)

    def rank(flag):
        down = turned(flag)
        return total(jnp.where(before, down, 0)), total(down)

    def ranked(flag, first):
        chosen, rest = jnp.where(flag & first, 1, 0), jnp.where(flag & ~first, 1, 0)
        (early, found), (late, _) = rank(chosen), rank(rest)
        return jnp.where(first, early, found + late)

    live = number < count
    half = lax.shift_right_logical(peer, 1)
    place = jnp.where((peer & 1) == 0, half, peers - 1 - half)
    low = table < table_count // 2
    away = jnp.where(low == first_ahead, at - place, place - at)
    away = jnp.where(away < 0, away + peers, away)
    key = jnp.where(live, peer * table_count + table, -1)
    order = jnp.where(low, ranked(low, live & (away == 1)), ranked(~low, live & (away == 1)))
    over = order >= cap
    spot = jnp.where(low, order, cap + order)
    spot = jnp.where(over, 2 * cap + ranked(over, live & (away == 2)), spot)

    slot = lax.broadcasted_iota(jnp.int32, (blocks, slots), 1)
    chosen = turned(spot)[:, :1] == slot
    down = lax.broadcasted_iota(jnp.int32, (blocks, slots), 0)

    def settled(row):
        return total(jnp.where(chosen, turned(row)[:, :1], 0))

    ordered_key = settled(key + 1) - 1
    ordered_down = turned(ordered_key)
    earlier = lax.broadcasted_iota(jnp.int32, (slots, slots), 0)
    later = lax.broadcasted_iota(jnp.int32, (slots, slots), 1)
    known = jnp.where((ordered_down == ordered_key) & (earlier < later), earlier, -1)
    known = jnp.max(known, axis=0, keepdims=True)
    tiles = peers * table_count
    wanted = lax.broadcasted_iota(jnp.int32, (slots, tiles), 1)
    ordinal = lax.broadcasted_iota(jnp.int32, (slots, tiles), 0)
    latest = jnp.max(
        jnp.where(ordered_down[:, :1] == wanted, ordinal, -1), axis=0, keepdims=True
    )
    plan_ref[0:1, :slots] = total(jnp.where(chosen, down, 0))
    plan_ref[1:2, :slots] = settled(jnp.where(low, table, table - table_count // 2))
    plan_ref[2:3, :slots] = settled(jnp.where(live, length, 0))
    plan_ref[3:4, :slots] = jnp.where(known < 0, slots, known)
    plan_ref[4:5, :tiles] = jnp.where(latest < 0, slots, latest)
    plan_ref[5:6, :slots] = settled(jnp.where(low, 0, 1))


def fused_kernel(
    peers,
    cap,
    share,
    count_ref,
    table_hbm,
    peer_hbm,
    len_hbm,
    rows_hbm,
    slots_hbm,
    tables_hbm,
    in_ref,
    out_w_ref,
    mix_hbm,
    bias_hbm,
    gate_hbm,
    result_ref,
    table_row,
    peer_row,
    len_row,
    rows_ref,
    slots_ref,
    mix_ref,
    bias_ref,
    gate_ref,
    plan_ref,
    index_ref,
    low_ref,
    high_ref,
    made_ref,
    first,
    held,
    emb,
    win,
    wout,
    small_sem,
    table_sem,
    ring_send,
    ring_recv,
    w_send,
    w_recv,
    w_local,
    half_send,
    half_recv,
):
    table_count, rows_dev, width = tables_hbm.shape
    blocks, block = rows_ref.shape
    slots = blocks + cap
    samples = result_ref.shape[0]
    part = table_count // RING
    experts = mix_ref.shape[0]
    pieces = 2 * experts
    me = lax.axis_index("mp")
    half = peers // 2
    at = jnp.where(lax.rem(me, 2) == 0, lax.div(me, 2), peers - 1 - lax.div(me, 2))
    d = lax.axis_index("dp")
    twin = d + 1 - 2 * lax.rem(d, 2)
    across = lax.rem(d + 2, 4)

    def member(position):
        position = lax.rem(position + 2 * peers, peers)
        return jnp.where(position < half, 2 * position, 2 * (peers - 1 - position) + 1)

    ahead, behind = member(at + 1), member(at - 1)
    beside = me + 1 - 2 * lax.rem(me, 2)
    first_ahead = lax.rem(d, 2) == 0
    targets = jnp.where(first_ahead, ahead, behind), jnp.where(first_ahead, behind, ahead)
    signs = jnp.where(first_ahead, 1, -1), jnp.where(first_ahead, -1, 1)

    pairs = (
        (table_hbm, table_row),
        (peer_hbm, peer_row),
        (len_hbm, len_row),
        (rows_hbm, rows_ref),
        (slots_hbm, slots_ref),
        (mix_hbm, mix_ref),
        (bias_hbm, bias_ref),
        (gate_hbm, gate_ref),
        (plan_ref, index_ref),
    )
    small = [pltpu.make_async_copy(a, b, small_sem.at[i]) for i, (a, b) in enumerate(pairs)]
    for copy in small[:5]:
        copy.start()
    half_tables = table_count // 2
    table_copies = [
        pltpu.make_async_copy(tables_hbm.at[t], place.at[t % half_tables], table_sem.at[t])
        for place, start in ((low_ref, 0), (high_ref, half_tables))
        for t in range(start, start + half_tables)
    ]
    for copy in table_copies:
        copy.start(priority=1)
    barrier = pltpu.get_barrier_semaphore()
    greet = [{"mp": ahead}, {"mp": behind}, {"dp": twin}, {"dp": across}]
    if share:
        greet.append({"mp": beside})
    for target in greet:
        pl.semaphore_signal(barrier, inc=1, device_id=target, device_id_type=MESH)
    made_ref[slots] = jnp.zeros((samples, width), jnp.float32)
    for copy in small[:5]:
        copy.wait()
    order_blocks(
        peers,
        table_count,
        cap,
        first_ahead,
        at,
        count_ref[0],
        table_row[...],
        peer_row[...],
        len_row[...],
        plan_ref,
    )
    small[8].start()
    pl.semaphore_wait(barrier, len(greet))

    def piece_refs(q, owner):
        if q < experts:
            return in_ref.at[q], win.at[owner, q]
        return out_w_ref.at[q - experts], wout.at[owner, q - experts]

    depth = in_ref.shape[1]
    mine = pl.ds(pl.multiple_of(lax.rem(me, 2) * (share // 2), 16), share // 2)
    halves = []
    if share:
        there = win.at[d, 0, mine]
        here = win.at[across, 0, mine]
        halves = [
            pltpu.make_async_remote_copy(
                src_ref=source,
                dst_ref=place,
                send_sem=half_send.at[n],
                recv_sem=half_recv.at[n],
                device_id=target,
                device_id_type=MESH,
            )
            for n, (source, place, target) in enumerate(
                ((in_ref.at[0, mine], there, {"dp": across}), (here, here, {"mp": beside}))
            )
        ]
        halves[0].start()

    def w_copy(kind, q):
        source, place = piece_refs(q, across if kind == 2 else d)
        if kind == 0 and q == 0 and share:
            rest = pl.ds(share, depth - share)
            source, place = source.at[rest], place.at[rest]
        return pltpu.make_async_remote_copy(
            src_ref=place if kind == 2 else source,
            dst_ref=place,
            send_sem=w_send.at[kind, q],
            recv_sem=w_recv.at[kind, q],
            device_id={"dp": across if kind == 0 else twin},
            device_id_type=MESH,
        )

    for q in range(1 if share == depth else 0, pieces):
        w_copy(0, q).start()
    for copy in small[5:8]:
        copy.start()

    def ring_copy(stream, source, step):
        target = targets[stream % 2]
        return pltpu.make_async_remote_copy(
            src_ref=source,
            dst_ref=held.at[step, stream],
            send_sem=ring_send.at[stream, step],
            recv_sem=ring_recv.at[stream, step],
            device_id={"mp": target},
            device_id_type=MESH,
        )

    def base(stream):
        return stream % 2 * (table_count // 2) + stream // 2 * part

    def own_tile(stream, distance, i):
        dest = member(at - signs[stream % 2] * distance)
        return made_ref[index_ref[4, dest * table_count + base(stream) + i]]

    even = rows_dev & (rows_dev - 1) == 0 and rows_dev >= FOLD * 128
    fold = FOLD if even else 1
    depth_rows = rows_dev // fold
    lane = lax.broadcasted_iota(jnp.int32, (block, 128), 1)
    sample = lax.broadcasted_iota(jnp.int32, (samples, block), 0)
    entry = lax.broadcasted_iota(jnp.int32, (samples, block), 1)

    def group(kind, g, carry):
        made = []
        for u in range(GROUP):
            b = g * GROUP + u
            source = index_ref[0, b]
            table = index_ref[1, b]
            column = jnp.broadcast_to(rows_ref[pl.ds(source, 1), :], (128, block)).T
            low = column & (depth_rows - 1) if even else column
            high = lax.shift_right_logical(column, depth_rows.bit_length() - 1)
            pick = jnp.concatenate(
                [
                    jnp.where(low == lane + c * 128, 1.0, 0.0).astype(jnp.bfloat16)
                    for c in range(depth_rows // 128)
                ],
                axis=1,
            )
            sides = []
            for j in range(fold):
                rows = slice(j * depth_rows, (j + 1) * depth_rows)
                if kind == 0:
                    sides.append(low_ref[table, rows, :])
                elif kind == 1:
                    sides.append(high_ref[table, rows, :])
                else:
                    upper = index_ref[5, b] == 1
                    sides.append(
                        jnp.where(upper, high_ref[table, rows, :], low_ref[table, rows, :])
                    )
            side = jnp.concatenate(sides, axis=1)
            wide = jnp.dot(pick, side, preferred_element_type=jnp.float32)
            picked = wide[:, :width]
            for j in range(1, fold):
                picked = jnp.where(high == j, wide[:, j * width : (j + 1) * width], picked)
            slot = slots_ref[pl.ds(source, 1), :]
            place = jnp.where((sample == slot) & (entry < index_ref[2, b]), 1.0, 0.0)
            made.append(
                jnp.dot(
                    place.astype(jnp.bfloat16),
                    picked.astype(jnp.bfloat16),
                    preferred_element_type=jnp.float32,
                )
            )
        for u in range(GROUP):
            b = g * GROUP + u
            made_ref[b] = made[u] + made_ref[index_ref[3, b]]
        return carry

    def pool(kind, start, end):
        work = functools.partial(group, kind)
        lax.fori_loop(start // GROUP, end // GROUP, work, 0)

    def begin(parity):
        for stream in range(parity, RING, 2):
            for i in range(part):
                first[stream, i] = own_tile(stream, 1, i).astype(jnp.bfloat16)
            ring_copy(stream, first.at[stream], 0).start()

    small[8].wait()
    for copy in table_copies[:half_tables]:
        copy.wait()
    pool(0, 0, cap)
    begin(0)
    for copy in table_copies[half_tables:]:
        copy.wait()
    pool(1, cap, 2 * cap)
    begin(1)
    if share:
        halves[0].wait_recv()
        halves[1].start()
    for q in range(pieces):
        w_copy(1, q).start()
    local = []
    for q in range(pieces):
        source, place = piece_refs(q, d)
        local.append(pltpu.make_async_copy(source, place, w_local.at[q]))
        local[-1].start()
    pool(2, 2 * cap, 4 * cap)

    gated = [jnp.zeros((samples, experts), jnp.float32)]
    projected = [jnp.zeros((samples, in_ref.shape[2]), jnp.float32) for _ in range(experts)]

    def hop(step, last):
        for stream in range(RING):
            ring_copy(stream, held.at[step, stream], step).wait_recv()
            for i in range(part):
                total = held[step, stream, i].astype(jnp.float32) + own_tile(stream, step + 2, i)
                total = total.astype(jnp.bfloat16)
                if last:
                    column = (base(stream) + i) * width
                    emb[:, column : column + width] = total
                else:
                    held[step, stream, i] = total
            if not last:
                ring_copy(stream, held.at[step, stream], step + 1).start()
                continue
            start, end = base(stream) * width, (base(stream) + part) * width
            while start < end:
                owner = start // depth
                stop = min(end, (owner + 1) * depth)
                ready = emb[:, start:stop]
                gated[0] += lax.dot_general(
                    ready,
                    gate_ref[:, start:stop],
                    (((1,), (1,)), ((), ())),
                    preferred_element_type=jnp.float32,
                )
                rows = slice(start - owner * depth, stop - owner * depth)
                for e in range(experts):
                    projected[e] += jnp.dot(
                        ready, win[owner, e, rows, :], preferred_element_type=jnp.float32
                    )
                start = stop

    def forward(first_piece, end_piece):
        for q in range(first_piece, end_piece):
            if q == 0 and share:
                halves[1].wait_recv()
            if q or share < depth:
                w_copy(0, q).wait_recv()
            w_copy(2, q).start()

    for step in range(peers - 2):
        hop(step, False)
        if step == 0:
            pool(2, 4 * cap, slots)
        forward(min(step, pieces - 1), min(step + 1, pieces - 1))
    forward(min(peers - 2, pieces - 1), pieces - 1)
    for copy in local:
        copy.wait()
    for copy in small[5:8]:
        copy.wait()
    for e in range(experts):
        w_copy(1, e).wait_recv()
        w_copy(2, e).wait_recv()
    hop(peers - 2, True)

    columns = out_w_ref.shape[2]
    gate = jax.nn.sigmoid(gated[0])
    mixed = []
    for e in range(experts):
        hidden = jnp.tanh(projected[e]).astype(jnp.bfloat16)
        mixed.append(
            jnp.tanh(
                jnp.dot(hidden, mix_ref[e], preferred_element_type=jnp.float32)
            ).astype(jnp.bfloat16)
        )

    def span(owner):
        return pl.ds(pl.multiple_of(owner * columns, 128), columns)

    def grown(owner, e):
        wide = jnp.dot(mixed[e], wout[owner, e], preferred_element_type=jnp.float32)
        return gate[:, e : e + 1] * (wide + bias_ref[e : e + 1, span(owner)])

    def finish(owner, weighted):
        base = emb[:, span(owner)].astype(jnp.float32)
        result_ref[:, span(owner)] = (base + base * weighted).astype(jnp.bfloat16)

    for e in range(experts):
        w_copy(1, experts + e).wait_recv()
    for owner in (d, twin):
        weighted = grown(owner, 0)
        for e in range(1, experts):
            weighted += grown(owner, e)
        finish(owner, weighted)
    forward(pieces - 1, pieces)
    for e in range(experts - 1):
        w_copy(2, experts + e).wait_recv()
    far = across + 1 - 2 * lax.rem(across, 2)
    pair = []
    for owner in (across, far):
        weighted = grown(owner, 0)
        for e in range(1, experts - 1):
            weighted += grown(owner, e)
        pair.append(weighted)
    finish(across, pair[0] + grown(across, experts - 1))
    w_copy(2, pieces - 1).wait_recv()
    finish(far, pair[1] + grown(far, experts - 1))

    for stream in range(RING):
        ring_copy(stream, first.at[stream], 0).wait_send()

    def sent(step, carry):
        for stream in range(RING):
            ring_copy(stream, held.at[step - 1, stream], step).wait_send()
        return carry

    lax.fori_loop(1, peers - 1, sent, 0)
    for copy in halves:
        copy.wait_send()
    for kind in (0, 1, 2):
        for q in range(1 if kind == 0 and share == depth else 0, pieces):
            w_copy(kind, q).wait_send()


def fused(
    peers,
    groups,
    tables,
    block_rows,
    block_slots,
    block_table,
    block_peer,
    block_len,
    block_count,
    cross_in,
    cross_mix,
    cross_out,
    cross_bias,
    gate_weight,
):
    table_count, _, width = tables.shape
    blocks = block_rows.shape[0]
    experts = cross_in.shape[0]
    cap = 2 * blocks // peers
    depth = cross_in.shape[1]
    share = SHARE if depth % 32 == 0 and SHARE <= depth else 0
    part = table_count // RING
    hbm = pl.BlockSpec(memory_space=pltpu.HBM)
    vmem = pl.BlockSpec(memory_space=pltpu.VMEM)
    lanes = -(-max(blocks + cap, peers * table_count) // 128) * 128
    operands = (
        block_table.reshape(1, blocks),
        block_peer.reshape(1, blocks),
        block_len.reshape(1, blocks),
        block_rows,
        block_slots,
        tables,
        cross_in,
        cross_out,
        cross_mix,
        cross_bias,
        gate_weight,
    )
    return pl.pallas_call(
        functools.partial(fused_kernel, peers, cap, share),
        out_shape=jax.ShapeDtypeStruct((B_DEV, table_count * width), jnp.bfloat16),
        in_specs=[pl.BlockSpec(memory_space=pltpu.SMEM)] + [hbm] * len(operands),
        out_specs=vmem,
        scratch_shapes=[
            pltpu.VMEM((1, blocks), jnp.int32),
            pltpu.VMEM((1, blocks), jnp.int32),
            pltpu.VMEM((1, blocks), jnp.int32),
            pltpu.VMEM(block_rows.shape, jnp.int32),
            pltpu.VMEM(block_slots.shape, jnp.int32),
            pltpu.VMEM(cross_mix.shape, jnp.bfloat16),
            pltpu.VMEM(cross_bias.shape, jnp.float32),
            pltpu.VMEM(gate_weight.shape, jnp.bfloat16),
            pltpu.VMEM((8, lanes), jnp.int32),
            pltpu.SMEM((8, lanes), jnp.int32),
            pltpu.VMEM((table_count // 2, *tables.shape[1:]), jnp.bfloat16),
            pltpu.VMEM((table_count // 2, *tables.shape[1:]), jnp.bfloat16),
            pltpu.VMEM((blocks + cap + 1, B_DEV, width), jnp.float32),
            pltpu.VMEM((RING, part, B_DEV, width), jnp.bfloat16),
            pltpu.VMEM((peers - 1, RING, part, B_DEV, width), jnp.bfloat16),
            pltpu.VMEM((B_DEV, table_count * width), jnp.bfloat16),
            pltpu.VMEM((groups, *cross_in.shape), jnp.bfloat16),
            pltpu.VMEM((groups, *cross_out.shape), jnp.bfloat16),
            pltpu.SemaphoreType.DMA((9,)),
            pltpu.SemaphoreType.DMA((table_count,)),
            pltpu.SemaphoreType.DMA((RING, peers - 1)),
            pltpu.SemaphoreType.DMA((RING, peers - 1)),
            pltpu.SemaphoreType.DMA((3, 2 * experts)),
            pltpu.SemaphoreType.DMA((3, 2 * experts)),
            pltpu.SemaphoreType.DMA((2 * experts,)),
            pltpu.SemaphoreType.DMA((2,)),
            pltpu.SemaphoreType.DMA((2,)),
        ],
        compiler_params=pltpu.CompilerParams(
            collective_id=0,
            has_side_effects=True,
            vmem_limit_bytes=FUSED_LIMIT,
        ),
        name="fused",
    )(block_count, *(pltpu.with_memory_space_constraint(x, pltpu.HBM) for x in operands))


def shared(peers, groups, cross_out):
    return groups == 4 and cross_out.shape[2] % 128 == 0 and peers <= 8


def cross(peers, groups, partial, cross_in, cross_mix, cross_out, cross_bias, gate_weight):
    tiles, samples, width = partial.shape
    table_count = tiles // peers
    cross_in = lax.all_gather(cross_in, "dp", axis=1, tiled=True)
    cross_out = lax.all_gather(cross_out, "dp", axis=2, tiled=True)
    vmem = pl.BlockSpec(memory_space=pltpu.VMEM)
    return pl.pallas_call(
        functools.partial(cross_kernel, peers),
        out_shape=jax.ShapeDtypeStruct((samples, table_count * width), jnp.bfloat16),
        in_specs=[vmem] * 6,
        out_specs=vmem,
        scratch_shapes=[
            pltpu.VMEM((peers - 1, STREAMS, table_count // STREAMS, samples, width), jnp.bfloat16),
            pltpu.VMEM((samples, table_count * width), jnp.bfloat16),
            pltpu.SemaphoreType.DMA((STREAMS, peers - 1)),
            pltpu.SemaphoreType.DMA((STREAMS, peers - 1)),
        ],
        compiler_params=pltpu.CompilerParams(
            collective_id=0,
            has_side_effects=True,
            vmem_limit_bytes=VMEM_LIMIT,
        ),
        name="cross",
    )(partial, cross_in, cross_mix, cross_out, cross_bias, gate_weight)


def on_device(
    tables,
    block_rows,
    block_slots,
    block_table,
    block_peer,
    block_len,
    block_count,
    cross_in,
    cross_mix,
    cross_out,
    cross_bias,
    gate_weight,
):
    peers, groups = lax.axis_size("mp"), lax.axis_size("dp")
    whole_tables = tables.shape[0] % RING == 0 and cross_in.shape[1] % tables.shape[2] == 0
    cap = 2 * block_rows.shape[0] // peers
    even = cap % GROUP == 0 and block_rows.shape[0] == 4 * cap and whole_tables
    if shared(peers, groups, cross_out) and even:
        return fused(
            peers,
            groups,
            tables,
            block_rows,
            block_slots,
            block_table,
            block_peer,
            block_len,
            block_count,
            cross_in,
            cross_mix,
            cross_out,
            cross_bias,
            gate_weight,
        )
    partial = pool(
        peers, tables, block_rows, block_slots, block_table, block_peer, block_len, block_count
    )
    return cross(
        peers, groups, partial, cross_in, cross_mix, cross_out, cross_bias, gate_weight
    )


def solution(mesh):
    in_specs = (
        P(None, "mp", None),
        P(("mp", "dp"), None),
        P(("mp", "dp"), None),
        P(("mp", "dp")),
        P(("mp", "dp"), None),
        P(("mp", "dp")),
        P(("mp", "dp")),
        P(None, "dp", None),
        P(),
        P(None, None, "dp"),
        P(),
        P(),
    )
    out_specs = P(("mp", "dp"), None)
    return jax.shard_map(
        on_device, mesh=mesh, in_specs=in_specs, out_specs=out_specs, check_vma=False
    )
```

```python
import functools

import jax
import jax.numpy as jnp
from jax import lax
from jax.experimental import pallas as pl
from jax.experimental.pallas import tpu as pltpu
from jax.sharding import PartitionSpec as P

B_DEV = 128
UNROLL = 8
STREAMS = 4
MESH = pl.DeviceIdType.MESH
POOL_LIMIT = 30 << 20
FUSED_LIMIT = 48 << 20
FOLD = 4
RING = 4
GROUP = 16
SHARE = 320
VMEM_LIMIT = 67043328


def pool_kernel(
    unroll,
    count_ref,
    table_hbm,
    peer_hbm,
    len_hbm,
    rows_hbm,
    slots_hbm,
    tables_hbm,
    out_ref,
    table_ref,
    peer_ref,
    len_ref,
    rows_ref,
    slots_ref,
    tables_ref,
    acc,
    slot_of,
    key_of,
    ready,
    small_sem,
    table_sem,
):
    table_count, rows_dev, width = tables_ref.shape
    total_blocks, block = rows_ref.shape
    tiles, samples, _ = out_ref.shape
    pairs = (
        (table_hbm, table_ref),
        (peer_hbm, peer_ref),
        (len_hbm, len_ref),
        (rows_hbm, rows_ref),
        (slots_hbm, slots_ref),
    )
    small = [pltpu.make_async_copy(a, b, small_sem.at[i]) for i, (a, b) in enumerate(pairs)]
    for copy in small:
        copy.start()

    def table_copy(t):
        return pltpu.make_async_copy(tables_hbm.at[t], tables_ref.at[t], table_sem.at[t])

    for t in range(table_count):
        table_copy(t).start()
        ready[t] = 0

    def need(t):
        @pl.when(ready[t] == 0)
        def _():
            table_copy(t).wait()
            ready[t] = 1

    def clear(i, carry):
        out_ref[i] = jnp.zeros((samples, width), jnp.bfloat16)
        slot_of[i] = -1
        return carry

    lax.fori_loop(0, tiles, clear, 0)
    for copy in small:
        copy.wait()
    count = count_ref[0]

    lane = lax.broadcasted_iota(jnp.int32, (block, 128), 1)
    sample = lax.broadcasted_iota(jnp.int32, (samples, block), 0)
    entry = lax.broadcasted_iota(jnp.int32, (samples, block), 1)

    def group(g, used):
        made = []
        for u in range(unroll):
            need(table_ref[g * unroll + u])
        for u in range(unroll):
            b = g * unroll + u
            row = rows_ref[pl.ds(b, 1), :]
            slot = slots_ref[pl.ds(b, 1), :]
            table = table_ref[b]
            column = jnp.broadcast_to(row, (128, block)).T
            pick = jnp.concatenate(
                [
                    jnp.where(column == lane + c * 128, 1.0, 0.0).astype(jnp.bfloat16)
                    for c in range(rows_dev // 128)
                ],
                axis=1,
            )
            picked = jnp.dot(pick, tables_ref[table], preferred_element_type=jnp.float32)
            place = jnp.where((sample == slot) & (entry < len_ref[b]), 1.0, 0.0)
            made.append(
                jnp.dot(
                    place.astype(jnp.bfloat16),
                    picked.astype(jnp.bfloat16),
                    preferred_element_type=jnp.float32,
                )
            )
        for u in range(unroll):
            b = g * unroll + u
            key = peer_ref[b] * table_count + table_ref[b]
            live = b < count
            known = slot_of[key]
            first = known < 0
            at = jnp.where(live, jnp.where(first, used, known), total_blocks)
            acc[at] = jnp.where(first, made[u], acc[at] + made[u])
            slot_of[key] = jnp.where(live, at, known)
            key_of[at] = key
            used = used + jnp.where(live & first, 1, 0)
        return used

    used = lax.fori_loop(0, (count + unroll - 1) // unroll, group, 0)

    def flush(i, carry):
        out_ref[key_of[i]] = acc[i].astype(jnp.bfloat16)
        return carry

    lax.fori_loop(0, used, flush, 0)
    for t in range(table_count):
        need(t)


def pool(peers, tables, block_rows, block_slots, block_table, block_peer, block_len, block_count):
    table_count, _, width = tables.shape
    total_blocks = block_rows.shape[0]
    tiles = peers * table_count
    unroll = UNROLL if total_blocks % UNROLL == 0 else 1
    hbm = pl.BlockSpec(memory_space=pltpu.HBM)
    vmem = pl.BlockSpec(memory_space=pltpu.VMEM)
    return pl.pallas_call(
        functools.partial(pool_kernel, unroll),
        out_shape=jax.ShapeDtypeStruct((tiles, B_DEV, width), jnp.bfloat16),
        in_specs=[pl.BlockSpec(memory_space=pltpu.SMEM)] + [hbm] * 6,
        out_specs=vmem,
        scratch_shapes=[
            pltpu.SMEM((total_blocks,), jnp.int32),
            pltpu.SMEM((total_blocks,), jnp.int32),
            pltpu.SMEM((total_blocks,), jnp.int32),
            pltpu.VMEM(block_rows.shape, jnp.int32),
            pltpu.VMEM(block_slots.shape, jnp.int32),
            pltpu.VMEM(tables.shape, jnp.bfloat16),
            pltpu.VMEM((total_blocks + 1, B_DEV, width), jnp.float32),
            pltpu.SMEM((tiles,), jnp.int32),
            pltpu.SMEM((total_blocks + 1,), jnp.int32),
            pltpu.SMEM((table_count,), jnp.int32),
            pltpu.SemaphoreType.DMA((5,)),
            pltpu.SemaphoreType.DMA((table_count,)),
        ],
        compiler_params=pltpu.CompilerParams(
            vmem_limit_bytes=POOL_LIMIT if peers <= 8 else VMEM_LIMIT
        ),
        cost_estimate=pl.CostEstimate(
            flops=2 * total_blocks * B_DEV * tables.shape[1] * width,
            bytes_accessed=2 * tables.size + 2 * tiles * B_DEV * width,
            transcendentals=0,
        ),
        name="pool",
    )(
        block_count,
        *(
            pltpu.with_memory_space_constraint(x, pltpu.HBM)
            for x in (
                block_table,
                block_peer[:, 0],
                block_len,
                block_rows,
                block_slots,
                tables,
            )
        )
    )


def cross_kernel(
    peers,
    partial_ref,
    in_ref,
    mix_ref,
    out_w_ref,
    bias_ref,
    gate_ref,
    result_ref,
    held,
    emb,
    ring_send,
    ring_recv,
):
    tiles, samples, width = partial_ref.shape
    table_count = tiles // peers
    part = table_count // STREAMS
    experts = mix_ref.shape[0]
    me = lax.axis_index("mp")
    half = peers // 2
    at = jnp.where(lax.rem(me, 2) == 0, lax.div(me, 2), peers - 1 - lax.div(me, 2))

    def member(position):
        position = lax.rem(position + 2 * peers, peers)
        return jnp.where(position < half, 2 * position, 2 * (peers - 1 - position) + 1)

    ahead, behind = member(at + 1), member(at - 1)

    barrier = pltpu.get_barrier_semaphore()
    greet = [{"mp": ahead}, {"mp": behind}]
    for target in greet:
        pl.semaphore_signal(barrier, inc=1, device_id=target, device_id_type=MESH)
    pl.semaphore_wait(barrier, len(greet))

    def ring_copy(stream, source, step):
        target = ahead if stream % 2 == 0 else behind
        return pltpu.make_async_remote_copy(
            src_ref=source,
            dst_ref=held.at[step, stream],
            send_sem=ring_send.at[stream, step],
            recv_sem=ring_recv.at[stream, step],
            device_id={"mp": target},
            device_id_type=MESH,
        )

    def own_tiles(stream, distance):
        dest = member(at - distance if stream % 2 == 0 else at + distance)
        return pl.ds(dest * table_count + stream * part, part)

    for stream in range(STREAMS):
        ring_copy(stream, partial_ref.at[own_tiles(stream, 1)], 0).start()

    def hop(step, last):
        for stream in range(STREAMS):
            ring_copy(stream, held.at[step, stream], step).wait_recv()
            mine = partial_ref[own_tiles(stream, step + 2)]
            total = held[step, stream].astype(jnp.float32) + mine.astype(jnp.float32)
            total = total.astype(jnp.bfloat16)
            if last:
                for i in range(part):
                    column = (stream * part + i) * width
                    emb[:, column : column + width] = total[i]
            else:
                held[step, stream] = total
                ring_copy(stream, held.at[step, stream], step + 1).start()

    def turn(step, carry):
        hop(step, False)
        return carry

    lax.fori_loop(0, peers - 2, turn, 0)
    hop(peers - 2, True)

    gate = jax.nn.sigmoid(
        lax.dot_general(
            emb[...], gate_ref[...], (((1,), (1,)), ((), ())), preferred_element_type=jnp.float32
        )
    )
    mixed = []
    for e in range(experts):
        projected = jnp.dot(emb[...], in_ref[e], preferred_element_type=jnp.float32)
        hidden = jnp.tanh(projected).astype(jnp.bfloat16)
        mixed.append(
            jnp.tanh(
                jnp.dot(hidden, mix_ref[e], preferred_element_type=jnp.float32)
            ).astype(jnp.bfloat16)
        )
    weighted = jnp.zeros(emb.shape, jnp.float32)
    for e in range(experts):
        grown = jnp.dot(mixed[e], out_w_ref[e], preferred_element_type=jnp.float32)
        weighted += gate[:, e : e + 1] * (grown + bias_ref[e : e + 1, :])
    base = emb[...].astype(jnp.float32)
    result_ref[...] = (base + base * weighted).astype(jnp.bfloat16)

    for stream in range(STREAMS):
        ring_copy(stream, partial_ref.at[own_tiles(stream, 1)], 0).wait_send()

    def sent(step, carry):
        for stream in range(STREAMS):
            ring_copy(stream, held.at[step - 1, stream], step).wait_send()
        return carry

    lax.fori_loop(1, peers - 1, sent, 0)


def order_blocks(peers, table_count, cap, first_ahead, at, count, table, peer, length, plan_ref):
    blocks = table.shape[1]
    slots = blocks + cap
    number = lax.broadcasted_iota(jnp.int32, (1, blocks), 1)
    before = lax.broadcasted_iota(jnp.int32, (blocks, blocks), 0) < lax.broadcasted_iota(
        jnp.int32, (blocks, blocks), 1
    )

    def turned(row):
        size = row.shape[1]
        return jnp.broadcast_to(row, (size, size)).T

    def total(x):
        return jnp.sum(x, axis=0, keepdims=True)

    def rank(flag):
        down = turned(flag)
        return total(jnp.where(before, down, 0)), total(down)

    def ranked(flag, first):
        chosen, rest = jnp.where(flag & first, 1, 0), jnp.where(flag & ~first, 1, 0)
        (early, found), (late, _) = rank(chosen), rank(rest)
        return jnp.where(first, early, found + late)

    live = number < count
    half = lax.shift_right_logical(peer, 1)
    place = jnp.where((peer & 1) == 0, half, peers - 1 - half)
    low = table < table_count // 2
    away = jnp.where(low == first_ahead, at - place, place - at)
    away = jnp.where(away < 0, away + peers, away)
    key = jnp.where(live, peer * table_count + table, -1)
    order = jnp.where(low, ranked(low, live & (away == 1)), ranked(~low, live & (away == 1)))
    over = order >= cap
    spot = jnp.where(low, order, cap + order)
    spot = jnp.where(over, 2 * cap + ranked(over, live & (away == 2)), spot)

    slot = lax.broadcasted_iota(jnp.int32, (blocks, slots), 1)
    chosen = turned(spot)[:, :1] == slot
    down = lax.broadcasted_iota(jnp.int32, (blocks, slots), 0)

    def settled(row):
        return total(jnp.where(chosen, turned(row)[:, :1], 0))

    ordered_key = settled(key + 1) - 1
    ordered_down = turned(ordered_key)
    earlier = lax.broadcasted_iota(jnp.int32, (slots, slots), 0)
    later = lax.broadcasted_iota(jnp.int32, (slots, slots), 1)
    known = jnp.where((ordered_down == ordered_key) & (earlier < later), earlier, -1)
    known = jnp.max(known, axis=0, keepdims=True)
    tiles = peers * table_count
    wanted = lax.broadcasted_iota(jnp.int32, (slots, tiles), 1)
    ordinal = lax.broadcasted_iota(jnp.int32, (slots, tiles), 0)
    latest = jnp.max(
        jnp.where(ordered_down[:, :1] == wanted, ordinal, -1), axis=0, keepdims=True
    )
    plan_ref[0:1, :slots] = total(jnp.where(chosen, down, 0))
    plan_ref[1:2, :slots] = settled(jnp.where(low, table, table - table_count // 2))
    plan_ref[2:3, :slots] = settled(jnp.where(live, length, 0))
    plan_ref[3:4, :slots] = jnp.where(known < 0, slots, known)
    plan_ref[4:5, :tiles] = jnp.where(latest < 0, slots, latest)
    plan_ref[5:6, :slots] = settled(jnp.where(low, 0, 1))


def fused_kernel(
    peers,
    cap,
    share,
    count_ref,
    table_hbm,
    peer_hbm,
    len_hbm,
    rows_hbm,
    slots_hbm,
    tables_hbm,
    in_ref,
    out_w_ref,
    mix_hbm,
    bias_hbm,
    gate_hbm,
    result_ref,
    table_row,
    peer_row,
    len_row,
    rows_ref,
    slots_ref,
    mix_ref,
    bias_ref,
    gate_ref,
    plan_ref,
    index_ref,
    low_ref,
    high_ref,
    made_ref,
    first,
    held,
    emb,
    win,
    wout,
    small_sem,
    table_sem,
    ring_send,
    ring_recv,
    w_send,
    w_recv,
    w_local,
    half_send,
    half_recv,
):
    table_count, rows_dev, width = tables_hbm.shape
    blocks, block = rows_ref.shape
    slots = blocks + cap
    samples = result_ref.shape[0]
    part = table_count // RING
    experts = mix_ref.shape[0]
    pieces = 2 * experts
    me = lax.axis_index("mp")
    half = peers // 2
    at = jnp.where(lax.rem(me, 2) == 0, lax.div(me, 2), peers - 1 - lax.div(me, 2))
    d = lax.axis_index("dp")
    twin = d + 1 - 2 * lax.rem(d, 2)
    across = lax.rem(d + 2, 4)

    def member(position):
        position = lax.rem(position + 2 * peers, peers)
        return jnp.where(position < half, 2 * position, 2 * (peers - 1 - position) + 1)

    ahead, behind = member(at + 1), member(at - 1)
    beside = me + 1 - 2 * lax.rem(me, 2)
    first_ahead = lax.rem(d, 2) == 0
    targets = jnp.where(first_ahead, ahead, behind), jnp.where(first_ahead, behind, ahead)
    signs = jnp.where(first_ahead, 1, -1), jnp.where(first_ahead, -1, 1)

    barrier = pltpu.get_barrier_semaphore()
    greet = [{"mp": ahead}, {"mp": behind}, {"dp": twin}, {"dp": across}]
    if share:
        greet.append({"mp": beside})
    for target in greet:
        pl.semaphore_signal(barrier, inc=1, device_id=target, device_id_type=MESH)
    pairs = (
        (table_hbm, table_row),
        (peer_hbm, peer_row),
        (len_hbm, len_row),
        (rows_hbm, rows_ref),
        (slots_hbm, slots_ref),
        (mix_hbm, mix_ref),
        (bias_hbm, bias_ref),
        (gate_hbm, gate_ref),
        (plan_ref, index_ref),
    )
    small = [pltpu.make_async_copy(a, b, small_sem.at[i]) for i, (a, b) in enumerate(pairs)]
    for copy in small[:5]:
        copy.start()
    half_tables = table_count // 2
    table_copies = [
        pltpu.make_async_copy(tables_hbm.at[t], place.at[t % half_tables], table_sem.at[t])
        for place, start in ((low_ref, 0), (high_ref, half_tables))
        for t in range(start, start + half_tables)
    ]
    for copy in table_copies:
        copy.start(priority=1)
    made_ref[slots] = jnp.zeros((samples, width), jnp.float32)
    for copy in small[:5]:
        copy.wait()
    order_blocks(
        peers,
        table_count,
        cap,
        first_ahead,
        at,
        count_ref[0],
        table_row[...],
        peer_row[...],
        len_row[...],
        plan_ref,
    )
    small[8].start()
    pl.semaphore_wait(barrier, len(greet))

    def piece_refs(q, owner):
        if q < experts:
            return in_ref.at[q], win.at[owner, q]
        return out_w_ref.at[q - experts], wout.at[owner, q - experts]

    depth = in_ref.shape[1]
    mine = pl.ds(pl.multiple_of(lax.rem(me, 2) * (share // 2), 16), share // 2)
    halves = []
    if share:
        there = win.at[d, 0, mine]
        here = win.at[across, 0, mine]
        halves = [
            pltpu.make_async_remote_copy(
                src_ref=source,
                dst_ref=place,
                send_sem=half_send.at[n],
                recv_sem=half_recv.at[n],
                device_id=target,
                device_id_type=MESH,
            )
            for n, (source, place, target) in enumerate(
                ((in_ref.at[0, mine], there, {"dp": across}), (here, here, {"mp": beside}))
            )
        ]
        halves[0].start()

    def w_copy(kind, q):
        source, place = piece_refs(q, across if kind == 2 else d)
        if kind == 0 and q == 0 and share:
            rest = pl.ds(share, depth - share)
            source, place = source.at[rest], place.at[rest]
        return pltpu.make_async_remote_copy(
            src_ref=place if kind == 2 else source,
            dst_ref=place,
            send_sem=w_send.at[kind, q],
            recv_sem=w_recv.at[kind, q],
            device_id={"dp": across if kind == 0 else twin},
            device_id_type=MESH,
        )

    for q in range(1 if share == depth else 0, pieces):
        w_copy(0, q).start()
    for copy in small[5:8]:
        copy.start()

    def ring_copy(stream, source, step):
        target = targets[stream % 2]
        return pltpu.make_async_remote_copy(
            src_ref=source,
            dst_ref=held.at[step, stream],
            send_sem=ring_send.at[stream, step],
            recv_sem=ring_recv.at[stream, step],
            device_id={"mp": target},
            device_id_type=MESH,
        )

    def base(stream):
        return stream % 2 * (table_count // 2) + stream // 2 * part

    def own_tile(stream, distance, i):
        dest = member(at - signs[stream % 2] * distance)
        return made_ref[index_ref[4, dest * table_count + base(stream) + i]]

    even = rows_dev & (rows_dev - 1) == 0 and rows_dev >= FOLD * 128
    fold = FOLD if even else 1
    depth_rows = rows_dev // fold
    lane = lax.broadcasted_iota(jnp.int32, (block, 128), 1)
    sample = lax.broadcasted_iota(jnp.int32, (samples, block), 0)
    entry = lax.broadcasted_iota(jnp.int32, (samples, block), 1)

    def group(kind, g, carry):
        made = []
        for u in range(GROUP):
            b = g * GROUP + u
            source = index_ref[0, b]
            table = index_ref[1, b]
            column = jnp.broadcast_to(rows_ref[pl.ds(source, 1), :], (128, block)).T
            low = column & (depth_rows - 1) if even else column
            high = lax.shift_right_logical(column, depth_rows.bit_length() - 1)
            pick = jnp.concatenate(
                [
                    jnp.where(low == lane + c * 128, 1.0, 0.0).astype(jnp.bfloat16)
                    for c in range(depth_rows // 128)
                ],
                axis=1,
            )
            sides = []
            for j in range(fold):
                rows = slice(j * depth_rows, (j + 1) * depth_rows)
                if kind == 0:
                    sides.append(low_ref[table, rows, :])
                elif kind == 1:
                    sides.append(high_ref[table, rows, :])
                else:
                    upper = index_ref[5, b] == 1
                    sides.append(
                        jnp.where(upper, high_ref[table, rows, :], low_ref[table, rows, :])
                    )
            side = jnp.concatenate(sides, axis=1)
            wide = jnp.dot(pick, side, preferred_element_type=jnp.float32)
            picked = wide[:, :width]
            for j in range(1, fold):
                picked = jnp.where(high == j, wide[:, j * width : (j + 1) * width], picked)
            slot = slots_ref[pl.ds(source, 1), :]
            place = jnp.where((sample == slot) & (entry < index_ref[2, b]), 1.0, 0.0)
            made.append(
                jnp.dot(
                    place.astype(jnp.bfloat16),
                    picked.astype(jnp.bfloat16),
                    preferred_element_type=jnp.float32,
                )
            )
        for u in range(GROUP):
            b = g * GROUP + u
            made_ref[b] = made[u] + made_ref[index_ref[3, b]]
        return carry

    def pool(kind, start, end):
        work = functools.partial(group, kind)
        lax.fori_loop(start // GROUP, end // GROUP, work, 0)

    def begin(parity):
        for stream in range(parity, RING, 2):
            for i in range(part):
                first[stream, i] = own_tile(stream, 1, i).astype(jnp.bfloat16)
            ring_copy(stream, first.at[stream], 0).start()

    small[8].wait()
    for copy in table_copies[:half_tables]:
        copy.wait()
    pool(0, 0, cap)
    begin(0)
    for copy in table_copies[half_tables:]:
        copy.wait()
    pool(1, cap, 2 * cap)
    begin(1)
    if share:
        halves[0].wait_recv()
        halves[1].start()
    for q in range(pieces):
        w_copy(1, q).start()
    local = []
    for q in range(pieces):
        source, place = piece_refs(q, d)
        local.append(pltpu.make_async_copy(source, place, w_local.at[q]))
        local[-1].start()
    pool(2, 2 * cap, 4 * cap)

    gated = [jnp.zeros((samples, experts), jnp.float32)]
    projected = [jnp.zeros((samples, in_ref.shape[2]), jnp.float32) for _ in range(experts)]

    def hop(step, last):
        for stream in range(RING):
            ring_copy(stream, held.at[step, stream], step).wait_recv()
            for i in range(part):
                total = held[step, stream, i].astype(jnp.float32) + own_tile(stream, step + 2, i)
                total = total.astype(jnp.bfloat16)
                if last:
                    column = (base(stream) + i) * width
                    emb[:, column : column + width] = total
                else:
                    held[step, stream, i] = total
            if not last:
                ring_copy(stream, held.at[step, stream], step + 1).start()
                continue
            start, end = base(stream) * width, (base(stream) + part) * width
            while start < end:
                owner = start // depth
                stop = min(end, (owner + 1) * depth)
                ready = emb[:, start:stop]
                gated[0] += lax.dot_general(
                    ready,
                    gate_ref[:, start:stop],
                    (((1,), (1,)), ((), ())),
                    preferred_element_type=jnp.float32,
                )
                rows = slice(start - owner * depth, stop - owner * depth)
                for e in range(experts):
                    projected[e] += jnp.dot(
                        ready, win[owner, e, rows, :], preferred_element_type=jnp.float32
                    )
                start = stop

    def forward(first_piece, end_piece):
        for q in range(first_piece, end_piece):
            if q == 0 and share:
                halves[1].wait_recv()
            if q or share < depth:
                w_copy(0, q).wait_recv()
            w_copy(2, q).start()

    for step in range(peers - 2):
        hop(step, False)
        if step == 0:
            pool(2, 4 * cap, slots)
        forward(min(step, pieces - 1), min(step + 1, pieces - 1))
    forward(min(peers - 2, pieces - 1), pieces - 1)
    for copy in local:
        copy.wait()
    for copy in small[5:8]:
        copy.wait()
    for e in range(experts):
        w_copy(1, e).wait_recv()
        w_copy(2, e).wait_recv()
    for stream in range(RING):
        ring_copy(stream, first.at[stream], 0).wait_send()

    def sent(step, carry):
        for stream in range(RING):
            ring_copy(stream, held.at[step - 1, stream], step).wait_send()
        return carry

    lax.fori_loop(1, peers - 2, sent, 0)
    for copy in halves:
        copy.wait_send()
    for q in range(1 if share == depth else 0, pieces - 1):
        w_copy(0, q).wait_send()
    for q in range(pieces):
        w_copy(1, q).wait_send()
    for q in range(pieces - 2):
        w_copy(2, q).wait_send()
    hop(peers - 2, True)

    columns = out_w_ref.shape[2]
    gate = jax.nn.sigmoid(gated[0])
    mixed = []
    for e in range(experts):
        hidden = jnp.tanh(projected[e]).astype(jnp.bfloat16)
        mixed.append(
            jnp.tanh(
                jnp.dot(hidden, mix_ref[e], preferred_element_type=jnp.float32)
            ).astype(jnp.bfloat16)
        )

    def span(owner):
        return pl.ds(pl.multiple_of(owner * columns, 128), columns)

    def grown(owner, e):
        wide = jnp.dot(mixed[e], wout[owner, e], preferred_element_type=jnp.float32)
        return gate[:, e : e + 1] * (wide + bias_ref[e : e + 1, span(owner)])

    def finish(owner, weighted):
        base = emb[:, span(owner)].astype(jnp.float32)
        result_ref[:, span(owner)] = (base + base * weighted).astype(jnp.bfloat16)

    forward(pieces - 1, pieces)
    for e in range(experts):
        w_copy(1, experts + e).wait_recv()
    for owner in (d, twin):
        weighted = grown(owner, 0)
        for e in range(1, experts):
            weighted += grown(owner, e)
        finish(owner, weighted)
    for e in range(experts - 1):
        w_copy(2, experts + e).wait_recv()
    far = across + 1 - 2 * lax.rem(across, 2)
    pair = []
    for owner in (across, far):
        weighted = grown(owner, 0)
        for e in range(1, experts - 1):
            weighted += grown(owner, e)
        pair.append(weighted)
    finish(across, pair[0] + grown(across, experts - 1))
    w_copy(2, pieces - 1).wait_recv()
    finish(far, pair[1] + grown(far, experts - 1))

    sent(peers - 2, 0)
    w_copy(0, pieces - 1).wait_send()
    w_copy(2, pieces - 2).wait_send()
    w_copy(2, pieces - 1).wait_send()


def fused(
    peers,
    groups,
    tables,
    block_rows,
    block_slots,
    block_table,
    block_peer,
    block_len,
    block_count,
    cross_in,
    cross_mix,
    cross_out,
    cross_bias,
    gate_weight,
):
    table_count, _, width = tables.shape
    blocks = block_rows.shape[0]
    experts = cross_in.shape[0]
    cap = 2 * blocks // peers
    depth = cross_in.shape[1]
    share = SHARE if depth % 32 == 0 and SHARE <= depth else 0
    part = table_count // RING
    hbm = pl.BlockSpec(memory_space=pltpu.HBM)
    vmem = pl.BlockSpec(memory_space=pltpu.VMEM)
    lanes = -(-max(blocks + cap, peers * table_count) // 128) * 128
    operands = (
        block_table.reshape(1, blocks),
        block_peer.reshape(1, blocks),
        block_len.reshape(1, blocks),
        block_rows,
        block_slots,
        tables,
        cross_in,
        cross_out,
        cross_mix,
        cross_bias,
        gate_weight,
    )
    return pl.pallas_call(
        functools.partial(fused_kernel, peers, cap, share),
        out_shape=jax.ShapeDtypeStruct((B_DEV, table_count * width), jnp.bfloat16),
        in_specs=[pl.BlockSpec(memory_space=pltpu.SMEM)] + [hbm] * len(operands),
        out_specs=vmem,
        scratch_shapes=[
            pltpu.VMEM((1, blocks), jnp.int32),
            pltpu.VMEM((1, blocks), jnp.int32),
            pltpu.VMEM((1, blocks), jnp.int32),
            pltpu.VMEM(block_rows.shape, jnp.int32),
            pltpu.VMEM(block_slots.shape, jnp.int32),
            pltpu.VMEM(cross_mix.shape, jnp.bfloat16),
            pltpu.VMEM(cross_bias.shape, jnp.float32),
            pltpu.VMEM(gate_weight.shape, jnp.bfloat16),
            pltpu.VMEM((8, lanes), jnp.int32),
            pltpu.SMEM((8, lanes), jnp.int32),
            pltpu.VMEM((table_count // 2, *tables.shape[1:]), jnp.bfloat16),
            pltpu.VMEM((table_count // 2, *tables.shape[1:]), jnp.bfloat16),
            pltpu.VMEM((blocks + cap + 1, B_DEV, width), jnp.float32),
            pltpu.VMEM((RING, part, B_DEV, width), jnp.bfloat16),
            pltpu.VMEM((peers - 1, RING, part, B_DEV, width), jnp.bfloat16),
            pltpu.VMEM((B_DEV, table_count * width), jnp.bfloat16),
            pltpu.VMEM((groups, *cross_in.shape), jnp.bfloat16),
            pltpu.VMEM((groups, *cross_out.shape), jnp.bfloat16),
            pltpu.SemaphoreType.DMA((9,)),
            pltpu.SemaphoreType.DMA((table_count,)),
            pltpu.SemaphoreType.DMA((RING, peers - 1)),
            pltpu.SemaphoreType.DMA((RING, peers - 1)),
            pltpu.SemaphoreType.DMA((3, 2 * experts)),
            pltpu.SemaphoreType.DMA((3, 2 * experts)),
            pltpu.SemaphoreType.DMA((2 * experts,)),
            pltpu.SemaphoreType.DMA((2,)),
            pltpu.SemaphoreType.DMA((2,)),
        ],
        compiler_params=pltpu.CompilerParams(
            collective_id=0,
            has_side_effects=True,
            vmem_limit_bytes=FUSED_LIMIT,
        ),
        name="fused",
    )(block_count, *(pltpu.with_memory_space_constraint(x, pltpu.HBM) for x in operands))


def shared(peers, groups, cross_out):
    return groups == 4 and cross_out.shape[2] % 128 == 0 and peers <= 8


def cross(peers, groups, partial, cross_in, cross_mix, cross_out, cross_bias, gate_weight):
    tiles, samples, width = partial.shape
    table_count = tiles // peers
    cross_in = lax.all_gather(cross_in, "dp", axis=1, tiled=True)
    cross_out = lax.all_gather(cross_out, "dp", axis=2, tiled=True)
    vmem = pl.BlockSpec(memory_space=pltpu.VMEM)
    return pl.pallas_call(
        functools.partial(cross_kernel, peers),
        out_shape=jax.ShapeDtypeStruct((samples, table_count * width), jnp.bfloat16),
        in_specs=[vmem] * 6,
        out_specs=vmem,
        scratch_shapes=[
            pltpu.VMEM((peers - 1, STREAMS, table_count // STREAMS, samples, width), jnp.bfloat16),
            pltpu.VMEM((samples, table_count * width), jnp.bfloat16),
            pltpu.SemaphoreType.DMA((STREAMS, peers - 1)),
            pltpu.SemaphoreType.DMA((STREAMS, peers - 1)),
        ],
        compiler_params=pltpu.CompilerParams(
            collective_id=0,
            has_side_effects=True,
            vmem_limit_bytes=VMEM_LIMIT,
        ),
        name="cross",
    )(partial, cross_in, cross_mix, cross_out, cross_bias, gate_weight)


def on_device(
    tables,
    block_rows,
    block_slots,
    block_table,
    block_peer,
    block_len,
    block_count,
    cross_in,
    cross_mix,
    cross_out,
    cross_bias,
    gate_weight,
):
    peers, groups = lax.axis_size("mp"), lax.axis_size("dp")
    whole_tables = tables.shape[0] % RING == 0 and cross_in.shape[1] % tables.shape[2] == 0
    cap = 2 * block_rows.shape[0] // peers
    even = cap % GROUP == 0 and block_rows.shape[0] == 4 * cap and whole_tables
    if shared(peers, groups, cross_out) and even:
        return fused(
            peers,
            groups,
            tables,
            block_rows,
            block_slots,
            block_table,
            block_peer,
            block_len,
            block_count,
            cross_in,
            cross_mix,
            cross_out,
            cross_bias,
            gate_weight,
        )
    partial = pool(
        peers, tables, block_rows, block_slots, block_table, block_peer, block_len, block_count
    )
    return cross(
        peers, groups, partial, cross_in, cross_mix, cross_out, cross_bias, gate_weight
    )


def solution(mesh):
    in_specs = (
        P(None, "mp", None),
        P(("mp", "dp"), None),
        P(("mp", "dp"), None),
        P(("mp", "dp")),
        P(("mp", "dp"), None),
        P(("mp", "dp")),
        P(("mp", "dp")),
        P(None, "dp", None),
        P(),
        P(None, None, "dp"),
        P(),
        P(),
    )
    out_specs = P(("mp", "dp"), None)
    return jax.shard_map(
        on_device, mesh=mesh, in_specs=in_specs, out_specs=out_specs, check_vma=False
    )
```

```python
import functools

import jax
import jax.numpy as jnp
from jax import lax
from jax.experimental import pallas as pl
from jax.experimental.pallas import tpu as pltpu
from jax.sharding import PartitionSpec as P

B_DEV = 128
UNROLL = 8
STREAMS = 4
MESH = pl.DeviceIdType.MESH
POOL_LIMIT = 30 << 20
FUSED_LIMIT = 48 << 20
FOLD = 4
RING = 4
GROUP = 16
SHARE = 320
VMEM_LIMIT = 67043328


def pool_kernel(
    unroll,
    count_ref,
    table_hbm,
    peer_hbm,
    len_hbm,
    rows_hbm,
    slots_hbm,
    tables_hbm,
    out_ref,
    table_ref,
    peer_ref,
    len_ref,
    rows_ref,
    slots_ref,
    tables_ref,
    acc,
    slot_of,
    key_of,
    ready,
    small_sem,
    table_sem,
):
    table_count, rows_dev, width = tables_ref.shape
    total_blocks, block = rows_ref.shape
    tiles, samples, _ = out_ref.shape
    pairs = (
        (table_hbm, table_ref),
        (peer_hbm, peer_ref),
        (len_hbm, len_ref),
        (rows_hbm, rows_ref),
        (slots_hbm, slots_ref),
    )
    small = [pltpu.make_async_copy(a, b, small_sem.at[i]) for i, (a, b) in enumerate(pairs)]
    for copy in small:
        copy.start()

    def table_copy(t):
        return pltpu.make_async_copy(tables_hbm.at[t], tables_ref.at[t], table_sem.at[t])

    for t in range(table_count):
        table_copy(t).start()
        ready[t] = 0

    def need(t):
        @pl.when(ready[t] == 0)
        def _():
            table_copy(t).wait()
            ready[t] = 1

    def clear(i, carry):
        out_ref[i] = jnp.zeros((samples, width), jnp.bfloat16)
        slot_of[i] = -1
        return carry

    lax.fori_loop(0, tiles, clear, 0)
    for copy in small:
        copy.wait()
    count = count_ref[0]

    lane = lax.broadcasted_iota(jnp.int32, (block, 128), 1)
    sample = lax.broadcasted_iota(jnp.int32, (samples, block), 0)
    entry = lax.broadcasted_iota(jnp.int32, (samples, block), 1)

    def group(g, used):
        made = []
        for u in range(unroll):
            need(table_ref[g * unroll + u])
        for u in range(unroll):
            b = g * unroll + u
            row = rows_ref[pl.ds(b, 1), :]
            slot = slots_ref[pl.ds(b, 1), :]
            table = table_ref[b]
            column = jnp.broadcast_to(row, (128, block)).T
            pick = jnp.concatenate(
                [
                    jnp.where(column == lane + c * 128, 1.0, 0.0).astype(jnp.bfloat16)
                    for c in range(rows_dev // 128)
                ],
                axis=1,
            )
            picked = jnp.dot(pick, tables_ref[table], preferred_element_type=jnp.float32)
            place = jnp.where((sample == slot) & (entry < len_ref[b]), 1.0, 0.0)
            made.append(
                jnp.dot(
                    place.astype(jnp.bfloat16),
                    picked.astype(jnp.bfloat16),
                    preferred_element_type=jnp.float32,
                )
            )
        for u in range(unroll):
            b = g * unroll + u
            key = peer_ref[b] * table_count + table_ref[b]
            live = b < count
            known = slot_of[key]
            first = known < 0
            at = jnp.where(live, jnp.where(first, used, known), total_blocks)
            acc[at] = jnp.where(first, made[u], acc[at] + made[u])
            slot_of[key] = jnp.where(live, at, known)
            key_of[at] = key
            used = used + jnp.where(live & first, 1, 0)
        return used

    used = lax.fori_loop(0, (count + unroll - 1) // unroll, group, 0)

    def flush(i, carry):
        out_ref[key_of[i]] = acc[i].astype(jnp.bfloat16)
        return carry

    lax.fori_loop(0, used, flush, 0)
    for t in range(table_count):
        need(t)


def pool(peers, tables, block_rows, block_slots, block_table, block_peer, block_len, block_count):
    table_count, _, width = tables.shape
    total_blocks = block_rows.shape[0]
    tiles = peers * table_count
    unroll = UNROLL if total_blocks % UNROLL == 0 else 1
    hbm = pl.BlockSpec(memory_space=pltpu.HBM)
    vmem = pl.BlockSpec(memory_space=pltpu.VMEM)
    return pl.pallas_call(
        functools.partial(pool_kernel, unroll),
        out_shape=jax.ShapeDtypeStruct((tiles, B_DEV, width), jnp.bfloat16),
        in_specs=[pl.BlockSpec(memory_space=pltpu.SMEM)] + [hbm] * 6,
        out_specs=vmem,
        scratch_shapes=[
            pltpu.SMEM((total_blocks,), jnp.int32),
            pltpu.SMEM((total_blocks,), jnp.int32),
            pltpu.SMEM((total_blocks,), jnp.int32),
            pltpu.VMEM(block_rows.shape, jnp.int32),
            pltpu.VMEM(block_slots.shape, jnp.int32),
            pltpu.VMEM(tables.shape, jnp.bfloat16),
            pltpu.VMEM((total_blocks + 1, B_DEV, width), jnp.float32),
            pltpu.SMEM((tiles,), jnp.int32),
            pltpu.SMEM((total_blocks + 1,), jnp.int32),
            pltpu.SMEM((table_count,), jnp.int32),
            pltpu.SemaphoreType.DMA((5,)),
            pltpu.SemaphoreType.DMA((table_count,)),
        ],
        compiler_params=pltpu.CompilerParams(
            vmem_limit_bytes=POOL_LIMIT if peers <= 8 else VMEM_LIMIT
        ),
        cost_estimate=pl.CostEstimate(
            flops=2 * total_blocks * B_DEV * tables.shape[1] * width,
            bytes_accessed=2 * tables.size + 2 * tiles * B_DEV * width,
            transcendentals=0,
        ),
        name="pool",
    )(
        block_count,
        *(
            pltpu.with_memory_space_constraint(x, pltpu.HBM)
            for x in (
                block_table,
                block_peer[:, 0],
                block_len,
                block_rows,
                block_slots,
                tables,
            )
        )
    )


def cross_kernel(
    peers,
    partial_ref,
    in_ref,
    mix_ref,
    out_w_ref,
    bias_ref,
    gate_ref,
    result_ref,
    held,
    emb,
    ring_send,
    ring_recv,
):
    tiles, samples, width = partial_ref.shape
    table_count = tiles // peers
    part = table_count // STREAMS
    experts = mix_ref.shape[0]
    me = lax.axis_index("mp")
    half = peers // 2
    at = jnp.where(lax.rem(me, 2) == 0, lax.div(me, 2), peers - 1 - lax.div(me, 2))

    def member(position):
        position = lax.rem(position + 2 * peers, peers)
        return jnp.where(position < half, 2 * position, 2 * (peers - 1 - position) + 1)

    ahead, behind = member(at + 1), member(at - 1)

    barrier = pltpu.get_barrier_semaphore()
    greet = [{"mp": ahead}, {"mp": behind}]
    for target in greet:
        pl.semaphore_signal(barrier, inc=1, device_id=target, device_id_type=MESH)
    pl.semaphore_wait(barrier, len(greet))

    def ring_copy(stream, source, step):
        target = ahead if stream % 2 == 0 else behind
        return pltpu.make_async_remote_copy(
            src_ref=source,
            dst_ref=held.at[step, stream],
            send_sem=ring_send.at[stream, step],
            recv_sem=ring_recv.at[stream, step],
            device_id={"mp": target},
            device_id_type=MESH,
        )

    def own_tiles(stream, distance):
        dest = member(at - distance if stream % 2 == 0 else at + distance)
        return pl.ds(dest * table_count + stream * part, part)

    for stream in range(STREAMS):
        ring_copy(stream, partial_ref.at[own_tiles(stream, 1)], 0).start()

    def hop(step, last):
        for stream in range(STREAMS):
            ring_copy(stream, held.at[step, stream], step).wait_recv()
            mine = partial_ref[own_tiles(stream, step + 2)]
            total = held[step, stream].astype(jnp.float32) + mine.astype(jnp.float32)
            total = total.astype(jnp.bfloat16)
            if last:
                for i in range(part):
                    column = (stream * part + i) * width
                    emb[:, column : column + width] = total[i]
            else:
                held[step, stream] = total
                ring_copy(stream, held.at[step, stream], step + 1).start()

    def turn(step, carry):
        hop(step, False)
        return carry

    lax.fori_loop(0, peers - 2, turn, 0)
    hop(peers - 2, True)

    gate = jax.nn.sigmoid(
        lax.dot_general(
            emb[...], gate_ref[...], (((1,), (1,)), ((), ())), preferred_element_type=jnp.float32
        )
    )
    mixed = []
    for e in range(experts):
        projected = jnp.dot(emb[...], in_ref[e], preferred_element_type=jnp.float32)
        hidden = jnp.tanh(projected).astype(jnp.bfloat16)
        mixed.append(
            jnp.tanh(
                jnp.dot(hidden, mix_ref[e], preferred_element_type=jnp.float32)
            ).astype(jnp.bfloat16)
        )
    weighted = jnp.zeros(emb.shape, jnp.float32)
    for e in range(experts):
        grown = jnp.dot(mixed[e], out_w_ref[e], preferred_element_type=jnp.float32)
        weighted += gate[:, e : e + 1] * (grown + bias_ref[e : e + 1, :])
    base = emb[...].astype(jnp.float32)
    result_ref[...] = (base + base * weighted).astype(jnp.bfloat16)

    for stream in range(STREAMS):
        ring_copy(stream, partial_ref.at[own_tiles(stream, 1)], 0).wait_send()

    def sent(step, carry):
        for stream in range(STREAMS):
            ring_copy(stream, held.at[step - 1, stream], step).wait_send()
        return carry

    lax.fori_loop(1, peers - 1, sent, 0)


def order_blocks(peers, table_count, cap, first_ahead, at, count, table, peer, length, plan_ref):
    blocks = table.shape[1]
    slots = blocks + cap
    number = lax.broadcasted_iota(jnp.int32, (1, blocks), 1)
    before = lax.broadcasted_iota(jnp.int32, (blocks, blocks), 0) < lax.broadcasted_iota(
        jnp.int32, (blocks, blocks), 1
    )

    def turned(row):
        size = row.shape[1]
        return jnp.broadcast_to(row, (size, size)).T

    def total(x):
        return jnp.sum(x, axis=0, keepdims=True)

    def rank(flag):
        down = turned(flag)
        return total(jnp.where(before, down, 0)), total(down)

    def ranked(flag, first):
        chosen, rest = jnp.where(flag & first, 1, 0), jnp.where(flag & ~first, 1, 0)
        (early, found), (late, _) = rank(chosen), rank(rest)
        return jnp.where(first, early, found + late)

    live = number < count
    half = lax.shift_right_logical(peer, 1)
    place = jnp.where((peer & 1) == 0, half, peers - 1 - half)
    low = table < table_count // 2
    away = jnp.where(low == first_ahead, at - place, place - at)
    away = jnp.where(away < 0, away + peers, away)
    key = jnp.where(live, peer * table_count + table, -1)
    order = jnp.where(low, ranked(low, live & (away == 1)), ranked(~low, live & (away == 1)))
    over = order >= cap
    spot = jnp.where(low, order, cap + order)
    spot = jnp.where(over, 2 * cap + ranked(over, live & (away == 2)), spot)

    slot = lax.broadcasted_iota(jnp.int32, (blocks, slots), 1)
    chosen = turned(spot)[:, :1] == slot
    down = lax.broadcasted_iota(jnp.int32, (blocks, slots), 0)

    def settled(row):
        return total(jnp.where(chosen, turned(row)[:, :1], 0))

    ordered_key = settled(key + 1) - 1
    ordered_down = turned(ordered_key)
    earlier = lax.broadcasted_iota(jnp.int32, (slots, slots), 0)
    later = lax.broadcasted_iota(jnp.int32, (slots, slots), 1)
    known = jnp.where((ordered_down == ordered_key) & (earlier < later), earlier, -1)
    known = jnp.max(known, axis=0, keepdims=True)
    tiles = peers * table_count
    wanted = lax.broadcasted_iota(jnp.int32, (slots, tiles), 1)
    ordinal = lax.broadcasted_iota(jnp.int32, (slots, tiles), 0)
    latest = jnp.max(
        jnp.where(ordered_down[:, :1] == wanted, ordinal, -1), axis=0, keepdims=True
    )
    plan_ref[0:1, :slots] = total(jnp.where(chosen, down, 0))
    plan_ref[1:2, :slots] = settled(jnp.where(low, table, table - table_count // 2))
    plan_ref[2:3, :slots] = settled(jnp.where(live, length, 0))
    plan_ref[3:4, :slots] = jnp.where(known < 0, slots, known)
    plan_ref[4:5, :tiles] = jnp.where(latest < 0, slots, latest)
    plan_ref[5:6, :slots] = settled(jnp.where(low, 0, 1))


def fused_kernel(
    peers,
    cap,
    share,
    count_ref,
    table_hbm,
    peer_hbm,
    len_hbm,
    rows_hbm,
    slots_hbm,
    tables_hbm,
    in_ref,
    out_w_ref,
    mix_hbm,
    bias_hbm,
    gate_hbm,
    result_ref,
    table_row,
    peer_row,
    len_row,
    rows_ref,
    slots_ref,
    mix_ref,
    bias_ref,
    gate_ref,
    plan_ref,
    index_ref,
    low_ref,
    high_ref,
    made_ref,
    first,
    held,
    emb,
    win,
    wout,
    small_sem,
    table_sem,
    ring_send,
    ring_recv,
    w_send,
    w_recv,
    w_local,
    half_send,
    half_recv,
):
    table_count, rows_dev, width = tables_hbm.shape
    blocks, block = rows_ref.shape
    slots = blocks + cap
    samples = result_ref.shape[0]
    part = table_count // RING
    experts = mix_ref.shape[0]
    pieces = 2 * experts + 1
    me = lax.axis_index("mp")
    half = peers // 2
    at = jnp.where(lax.rem(me, 2) == 0, lax.div(me, 2), peers - 1 - lax.div(me, 2))
    d = lax.axis_index("dp")
    twin = d + 1 - 2 * lax.rem(d, 2)
    across = lax.rem(d + 2, 4)

    def member(position):
        position = lax.rem(position + 2 * peers, peers)
        return jnp.where(position < half, 2 * position, 2 * (peers - 1 - position) + 1)

    ahead, behind = member(at + 1), member(at - 1)
    beside = me + 1 - 2 * lax.rem(me, 2)
    first_ahead = lax.rem(d, 2) == 0
    targets = jnp.where(first_ahead, ahead, behind), jnp.where(first_ahead, behind, ahead)
    signs = jnp.where(first_ahead, 1, -1), jnp.where(first_ahead, -1, 1)

    barrier = pltpu.get_barrier_semaphore()
    greet = [{"mp": ahead}, {"mp": behind}, {"dp": twin}, {"dp": across}]
    if share:
        greet.append({"mp": beside})
    for target in greet:
        pl.semaphore_signal(barrier, inc=1, device_id=target, device_id_type=MESH)
    pairs = (
        (table_hbm, table_row),
        (peer_hbm, peer_row),
        (len_hbm, len_row),
        (rows_hbm, rows_ref),
        (slots_hbm, slots_ref),
        (mix_hbm, mix_ref),
        (bias_hbm, bias_ref),
        (gate_hbm, gate_ref),
        (plan_ref, index_ref),
    )
    small = [pltpu.make_async_copy(a, b, small_sem.at[i]) for i, (a, b) in enumerate(pairs)]
    for copy in small[:5]:
        copy.start()
    half_tables = table_count // 2
    table_copies = [
        pltpu.make_async_copy(tables_hbm.at[t], place.at[t % half_tables], table_sem.at[t])
        for place, start in ((low_ref, 0), (high_ref, half_tables))
        for t in range(start, start + half_tables)
    ]
    for copy in table_copies:
        copy.start(priority=1)
    made_ref[slots] = jnp.zeros((samples, width), jnp.float32)
    for copy in small[:5]:
        copy.wait()
    order_blocks(
        peers,
        table_count,
        cap,
        first_ahead,
        at,
        count_ref[0],
        table_row[...],
        peer_row[...],
        len_row[...],
        plan_ref,
    )
    small[8].start()
    pl.semaphore_wait(barrier, len(greet))

    def piece_refs(q, owner):
        if q < experts:
            return in_ref.at[q], win.at[owner, q]
        if q < 2 * experts - 1:
            return out_w_ref.at[q - experts], wout.at[owner, q - experts]
        rank = out_w_ref.shape[1] // 2
        rows = pl.ds((q - 2 * experts + 1) * rank, rank)
        return out_w_ref.at[experts - 1, rows], wout.at[owner, experts - 1, rows]

    depth = in_ref.shape[1]
    mine = pl.ds(pl.multiple_of(lax.rem(me, 2) * (share // 2), 16), share // 2)
    halves = []
    if share:
        there = win.at[d, 0, mine]
        here = win.at[across, 0, mine]
        halves = [
            pltpu.make_async_remote_copy(
                src_ref=source,
                dst_ref=place,
                send_sem=half_send.at[n],
                recv_sem=half_recv.at[n],
                device_id=target,
                device_id_type=MESH,
            )
            for n, (source, place, target) in enumerate(
                ((in_ref.at[0, mine], there, {"dp": across}), (here, here, {"mp": beside}))
            )
        ]
        halves[0].start()

    def w_copy(kind, q):
        source, place = piece_refs(q, across if kind == 2 else d)
        if kind == 0 and q == 0 and share:
            rest = pl.ds(share, depth - share)
            source, place = source.at[rest], place.at[rest]
        return pltpu.make_async_remote_copy(
            src_ref=place if kind == 2 else source,
            dst_ref=place,
            send_sem=w_send.at[kind, q],
            recv_sem=w_recv.at[kind, q],
            device_id={"dp": across if kind == 0 else twin},
            device_id_type=MESH,
        )

    for q in range(1 if share == depth else 0, pieces):
        w_copy(0, q).start()
    for copy in small[5:8]:
        copy.start()

    def ring_copy(stream, source, step):
        target = targets[stream % 2]
        return pltpu.make_async_remote_copy(
            src_ref=source,
            dst_ref=held.at[step, stream],
            send_sem=ring_send.at[stream, step],
            recv_sem=ring_recv.at[stream, step],
            device_id={"mp": target},
            device_id_type=MESH,
        )

    def base(stream):
        return stream % 2 * (table_count // 2) + stream // 2 * part

    def own_tile(stream, distance, i):
        dest = member(at - signs[stream % 2] * distance)
        return made_ref[index_ref[4, dest * table_count + base(stream) + i]]

    even = rows_dev & (rows_dev - 1) == 0 and rows_dev >= FOLD * 128
    fold = FOLD if even else 1
    depth_rows = rows_dev // fold
    lane = lax.broadcasted_iota(jnp.int32, (block, 128), 1)
    sample = lax.broadcasted_iota(jnp.int32, (samples, block), 0)
    entry = lax.broadcasted_iota(jnp.int32, (samples, block), 1)

    def group(kind, g, carry):
        made = []
        for u in range(GROUP):
            b = g * GROUP + u
            source = index_ref[0, b]
            table = index_ref[1, b]
            column = jnp.broadcast_to(rows_ref[pl.ds(source, 1), :], (128, block)).T
            low = column & (depth_rows - 1) if even else column
            high = lax.shift_right_logical(column, depth_rows.bit_length() - 1)
            pick = jnp.concatenate(
                [
                    jnp.where(low == lane + c * 128, 1.0, 0.0).astype(jnp.bfloat16)
                    for c in range(depth_rows // 128)
                ],
                axis=1,
            )
            sides = []
            for j in range(fold):
                rows = slice(j * depth_rows, (j + 1) * depth_rows)
                if kind == 0:
                    sides.append(low_ref[table, rows, :])
                elif kind == 1:
                    sides.append(high_ref[table, rows, :])
                else:
                    upper = index_ref[5, b] == 1
                    sides.append(
                        jnp.where(upper, high_ref[table, rows, :], low_ref[table, rows, :])
                    )
            side = jnp.concatenate(sides, axis=1)
            wide = jnp.dot(pick, side, preferred_element_type=jnp.float32)
            picked = wide[:, :width]
            for j in range(1, fold):
                picked = jnp.where(high == j, wide[:, j * width : (j + 1) * width], picked)
            slot = slots_ref[pl.ds(source, 1), :]
            place = jnp.where((sample == slot) & (entry < index_ref[2, b]), 1.0, 0.0)
            made.append(
                jnp.dot(
                    place.astype(jnp.bfloat16),
                    picked.astype(jnp.bfloat16),
                    preferred_element_type=jnp.float32,
                )
            )
        for u in range(GROUP):
            b = g * GROUP + u
            made_ref[b] = made[u] + made_ref[index_ref[3, b]]
        return carry

    def pool(kind, start, end):
        work = functools.partial(group, kind)
        lax.fori_loop(start // GROUP, end // GROUP, work, 0)

    def begin(parity):
        for stream in range(parity, RING, 2):
            for i in range(part):
                first[stream, i] = own_tile(stream, 1, i).astype(jnp.bfloat16)
            ring_copy(stream, first.at[stream], 0).start()

    small[8].wait()
    for copy in table_copies[:half_tables]:
        copy.wait()
    pool(0, 0, cap)
    begin(0)
    for copy in table_copies[half_tables:]:
        copy.wait()
    pool(1, cap, 2 * cap)
    begin(1)
    if share:
        halves[0].wait_recv()
        halves[1].start()
    for q in range(pieces):
        w_copy(1, q).start()
    local = []
    for q in range(pieces):
        source, place = piece_refs(q, d)
        local.append(pltpu.make_async_copy(source, place, w_local.at[q]))
        local[-1].start()
    pool(2, 2 * cap, 4 * cap)

    gated = [jnp.zeros((samples, experts), jnp.float32)]
    projected = [jnp.zeros((samples, in_ref.shape[2]), jnp.float32) for _ in range(experts)]

    def hop(step, last):
        for stream in range(RING):
            ring_copy(stream, held.at[step, stream], step).wait_recv()
            for i in range(part):
                total = held[step, stream, i].astype(jnp.float32) + own_tile(stream, step + 2, i)
                total = total.astype(jnp.bfloat16)
                if last:
                    column = (base(stream) + i) * width
                    emb[:, column : column + width] = total
                else:
                    held[step, stream, i] = total
            if not last:
                ring_copy(stream, held.at[step, stream], step + 1).start()
                continue
            start, end = base(stream) * width, (base(stream) + part) * width
            while start < end:
                owner = start // depth
                stop = min(end, (owner + 1) * depth)
                ready = emb[:, start:stop]
                gated[0] += lax.dot_general(
                    ready,
                    gate_ref[:, start:stop],
                    (((1,), (1,)), ((), ())),
                    preferred_element_type=jnp.float32,
                )
                rows = slice(start - owner * depth, stop - owner * depth)
                for e in range(experts):
                    projected[e] += jnp.dot(
                        ready, win[owner, e, rows, :], preferred_element_type=jnp.float32
                    )
                start = stop

    def forward(first_piece, end_piece):
        for q in range(first_piece, end_piece):
            if q == 0 and share:
                halves[1].wait_recv()
            if q or share < depth:
                w_copy(0, q).wait_recv()
            w_copy(2, q).start()

    for step in range(peers - 2):
        hop(step, False)
        if step == 0:
            pool(2, 4 * cap, slots)
        forward(min(step, pieces - 2), min(step + 1, pieces - 2))
    forward(min(peers - 2, pieces - 2), pieces - 2)
    for copy in local:
        copy.wait()
    for copy in small[5:8]:
        copy.wait()
    for e in range(experts):
        w_copy(1, e).wait_recv()
        w_copy(2, e).wait_recv()
    for stream in range(RING):
        ring_copy(stream, first.at[stream], 0).wait_send()

    def sent(step, carry):
        for stream in range(RING):
            ring_copy(stream, held.at[step - 1, stream], step).wait_send()
        return carry

    lax.fori_loop(1, peers - 2, sent, 0)
    for copy in halves:
        copy.wait_send()
    for q in range(1 if share == depth else 0, pieces - 2):
        w_copy(0, q).wait_send()
    for q in range(pieces):
        w_copy(1, q).wait_send()
    for q in range(pieces - 3):
        w_copy(2, q).wait_send()
    hop(peers - 2, True)

    columns = out_w_ref.shape[2]
    gate = jax.nn.sigmoid(gated[0])
    mixed = []
    for e in range(experts):
        hidden = jnp.tanh(projected[e]).astype(jnp.bfloat16)
        mixed.append(
            jnp.tanh(
                jnp.dot(hidden, mix_ref[e], preferred_element_type=jnp.float32)
            ).astype(jnp.bfloat16)
        )

    def span(owner):
        return pl.ds(pl.multiple_of(owner * columns, 128), columns)

    def grown(owner, e):
        wide = jnp.dot(mixed[e], wout[owner, e], preferred_element_type=jnp.float32)
        return gate[:, e : e + 1] * (wide + bias_ref[e : e + 1, span(owner)])

    def finish(owner, weighted):
        base = emb[:, span(owner)].astype(jnp.float32)
        result_ref[:, span(owner)] = (base + base * weighted).astype(jnp.bfloat16)

    forward(pieces - 2, pieces)
    for q in range(experts, pieces):
        w_copy(1, q).wait_recv()
    for owner in (d, twin):
        weighted = grown(owner, 0)
        for e in range(1, experts):
            weighted += grown(owner, e)
        finish(owner, weighted)
    for e in range(experts - 1):
        w_copy(2, experts + e).wait_recv()
    far = across + 1 - 2 * lax.rem(across, 2)
    pair = []
    for owner in (across, far):
        weighted = grown(owner, 0)
        for e in range(1, experts - 1):
            weighted += grown(owner, e)
        pair.append(weighted)
    finish(across, pair[0] + grown(across, experts - 1))
    for q in range(pieces - 2, pieces):
        w_copy(2, q).wait_recv()
    finish(far, pair[1] + grown(far, experts - 1))

    sent(peers - 2, 0)
    for q in range(pieces - 2, pieces):
        w_copy(0, q).wait_send()
    for q in range(pieces - 3, pieces):
        w_copy(2, q).wait_send()


def fused(
    peers,
    groups,
    tables,
    block_rows,
    block_slots,
    block_table,
    block_peer,
    block_len,
    block_count,
    cross_in,
    cross_mix,
    cross_out,
    cross_bias,
    gate_weight,
):
    table_count, _, width = tables.shape
    blocks = block_rows.shape[0]
    experts = cross_in.shape[0]
    cap = 2 * blocks // peers
    depth = cross_in.shape[1]
    share = SHARE if depth % 32 == 0 and SHARE <= depth else 0
    part = table_count // RING
    hbm = pl.BlockSpec(memory_space=pltpu.HBM)
    vmem = pl.BlockSpec(memory_space=pltpu.VMEM)
    lanes = -(-max(blocks + cap, peers * table_count) // 128) * 128
    operands = (
        block_table.reshape(1, blocks),
        block_peer.reshape(1, blocks),
        block_len.reshape(1, blocks),
        block_rows,
        block_slots,
        tables,
        cross_in,
        cross_out,
        cross_mix,
        cross_bias,
        gate_weight,
    )
    return pl.pallas_call(
        functools.partial(fused_kernel, peers, cap, share),
        out_shape=jax.ShapeDtypeStruct((B_DEV, table_count * width), jnp.bfloat16),
        in_specs=[pl.BlockSpec(memory_space=pltpu.SMEM)] + [hbm] * len(operands),
        out_specs=vmem,
        scratch_shapes=[
            pltpu.VMEM((1, blocks), jnp.int32),
            pltpu.VMEM((1, blocks), jnp.int32),
            pltpu.VMEM((1, blocks), jnp.int32),
            pltpu.VMEM(block_rows.shape, jnp.int32),
            pltpu.VMEM(block_slots.shape, jnp.int32),
            pltpu.VMEM(cross_mix.shape, jnp.bfloat16),
            pltpu.VMEM(cross_bias.shape, jnp.float32),
            pltpu.VMEM(gate_weight.shape, jnp.bfloat16),
            pltpu.VMEM((8, lanes), jnp.int32),
            pltpu.SMEM((8, lanes), jnp.int32),
            pltpu.VMEM((table_count // 2, *tables.shape[1:]), jnp.bfloat16),
            pltpu.VMEM((table_count // 2, *tables.shape[1:]), jnp.bfloat16),
            pltpu.VMEM((blocks + cap + 1, B_DEV, width), jnp.float32),
            pltpu.VMEM((RING, part, B_DEV, width), jnp.bfloat16),
            pltpu.VMEM((peers - 1, RING, part, B_DEV, width), jnp.bfloat16),
            pltpu.VMEM((B_DEV, table_count * width), jnp.bfloat16),
            pltpu.VMEM((groups, *cross_in.shape), jnp.bfloat16),
            pltpu.VMEM((groups, *cross_out.shape), jnp.bfloat16),
            pltpu.SemaphoreType.DMA((9,)),
            pltpu.SemaphoreType.DMA((table_count,)),
            pltpu.SemaphoreType.DMA((RING, peers - 1)),
            pltpu.SemaphoreType.DMA((RING, peers - 1)),
            pltpu.SemaphoreType.DMA((3, 2 * experts + 1)),
            pltpu.SemaphoreType.DMA((3, 2 * experts + 1)),
            pltpu.SemaphoreType.DMA((2 * experts + 1,)),
            pltpu.SemaphoreType.DMA((2,)),
            pltpu.SemaphoreType.DMA((2,)),
        ],
        compiler_params=pltpu.CompilerParams(
            collective_id=0,
            has_side_effects=True,
            vmem_limit_bytes=FUSED_LIMIT,
        ),
        name="fused",
    )(block_count, *(pltpu.with_memory_space_constraint(x, pltpu.HBM) for x in operands))


def shared(peers, groups, cross_out):
    return groups == 4 and cross_out.shape[2] % 128 == 0 and peers <= 8


def cross(peers, groups, partial, cross_in, cross_mix, cross_out, cross_bias, gate_weight):
    tiles, samples, width = partial.shape
    table_count = tiles // peers
    cross_in = lax.all_gather(cross_in, "dp", axis=1, tiled=True)
    cross_out = lax.all_gather(cross_out, "dp", axis=2, tiled=True)
    vmem = pl.BlockSpec(memory_space=pltpu.VMEM)
    return pl.pallas_call(
        functools.partial(cross_kernel, peers),
        out_shape=jax.ShapeDtypeStruct((samples, table_count * width), jnp.bfloat16),
        in_specs=[vmem] * 6,
        out_specs=vmem,
        scratch_shapes=[
            pltpu.VMEM((peers - 1, STREAMS, table_count // STREAMS, samples, width), jnp.bfloat16),
            pltpu.VMEM((samples, table_count * width), jnp.bfloat16),
            pltpu.SemaphoreType.DMA((STREAMS, peers - 1)),
            pltpu.SemaphoreType.DMA((STREAMS, peers - 1)),
        ],
        compiler_params=pltpu.CompilerParams(
            collective_id=0,
            has_side_effects=True,
            vmem_limit_bytes=VMEM_LIMIT,
        ),
        name="cross",
    )(partial, cross_in, cross_mix, cross_out, cross_bias, gate_weight)


def on_device(
    tables,
    block_rows,
    block_slots,
    block_table,
    block_peer,
    block_len,
    block_count,
    cross_in,
    cross_mix,
    cross_out,
    cross_bias,
    gate_weight,
):
    peers, groups = lax.axis_size("mp"), lax.axis_size("dp")
    whole_tables = tables.shape[0] % RING == 0 and cross_in.shape[1] % tables.shape[2] == 0
    cap = 2 * block_rows.shape[0] // peers
    even = cap % GROUP == 0 and block_rows.shape[0] == 4 * cap and whole_tables
    if shared(peers, groups, cross_out) and even:
        return fused(
            peers,
            groups,
            tables,
            block_rows,
            block_slots,
            block_table,
            block_peer,
            block_len,
            block_count,
            cross_in,
            cross_mix,
            cross_out,
            cross_bias,
            gate_weight,
        )
    partial = pool(
        peers, tables, block_rows, block_slots, block_table, block_peer, block_len, block_count
    )
    return cross(
        peers, groups, partial, cross_in, cross_mix, cross_out, cross_bias, gate_weight
    )


def solution(mesh):
    in_specs = (
        P(None, "mp", None),
        P(("mp", "dp"), None),
        P(("mp", "dp"), None),
        P(("mp", "dp")),
        P(("mp", "dp"), None),
        P(("mp", "dp")),
        P(("mp", "dp")),
        P(None, "dp", None),
        P(),
        P(None, None, "dp"),
        P(),
        P(),
    )
    out_specs = P(("mp", "dp"), None)
    return jax.shard_map(
        on_device, mesh=mesh, in_specs=in_specs, out_specs=out_specs, check_vma=False
    )
```
